32 devices in a mesh: aa: 4 (over x, core), ba: 8 (over z, y).
Axes of the slice: x: 2, y: 2, z: 4, core: 2. Of those that a mesh axis runs over, the one named last changes fastest.
Arguments:
- activations: bfloat16 [1024, 4224], P('aa', 'ba'), may hold values from -6 to 6
- out_grad: bfloat16 [1024, 4096], P('aa', 'ba'), may hold values from -0.1875 to 0.1875
- momentum: float32 [4224, 4096], P('aa', 'ba'), may hold values from -6 to 6
- weight: float32 [4224, 4096], P('aa', 'ba'), may hold values from -6 to 6
- norm_scale: float32 [], replicated, may hold values from 128.99231 to 257.98462
- step_size: float32 [], replicated, may hold values from 0.5 to 2
Outputs:
- new_weight: float32 [4224, 4096], P('aa', 'ba')
- new_momentum: float32 [4224, 4096], P('aa', 'ba')
The draws below stay inside these ranges and needn't reach their ends.
All inputs are finite; a program needn't handle non-finite values.
Results may differ from the reference program's by a relative error of at most 0.00068.
Values may be sent and summed in bfloat16 or wider, within the bound.
A program may use at most 64 MiB of HBM per device.

```python
import math
import jax
import jax.numpy as jnp

ROWS = 4224
COLS = 4096
TOKENS = 1024


def strengthened(result, own_key, source, target, shards_of, factor):
    owner, partner = [(jnp.arange(result.shape[position]) // (result.shape[position] // shards_of)).reshape([-1 if axis == position else 1 for axis in range(result.ndim)]) for position in (source, target)]
    chosen = jax.random.permutation(own_key, shards_of)[partner]
    strong = (owner == chosen) | (owner == (partner + shards_of // 2) % shards_of)
    return jnp.where(strong, factor * result, result)


def steps_of(own_key, extent, cuts, least, high):
    level, own = 1.0, jax.random.fold_in(own_key, 6)
    for position, blocks in cuts:
        heights = jnp.exp(jax.random.uniform(jax.random.fold_in(own, position), (blocks,), jnp.float32, least / len(cuts), high / len(cuts)))
        level = level * jnp.repeat(heights, extent[position] // blocks).reshape([-1 if axis == position else 1 for axis in range(len(extent))])
    return level


def normal_values(own_key, shape, width, most, split=(), kind=jnp.bfloat16):
    array = width * jax.random.normal(own_key, shape, jnp.float32)
    if split:
        array = array * steps_of(own_key, shape, split, -0.22, 0.18)
    return jnp.clip(array, -most, most).astype(kind)


def gaussian_with(own_key, extent, width, limit, pieces, heavy, kind=jnp.bfloat16):
    drawn = width * jax.random.normal(own_key, extent, jnp.float32)
    if pieces:
        drawn = drawn * steps_of(own_key, extent, pieces, -0.22, 0.18)
    return jnp.clip(strengthened(drawn, jax.random.fold_in(own_key, 3), *heavy), -limit, limit).astype(kind)


def setup_inputs(seed: int = 0) -> dict:
    key_of = jax.random.split(jax.random.key(seed), 7)
    return {
        "activations": gaussian_with(key_of[0], (TOKENS, ROWS), 1.0, 6.0, ((0, 4), (1, 8)), (0, 1, 8, 2.0)),
        "out_grad": normal_values(key_of[1], (TOKENS, COLS), (TOKENS ** -0.5), 0.1875, ((0, 4), (1, 8))),
        "momentum": normal_values(key_of[2], (ROWS, COLS), 1.0, 6.0, ((0, 4), (1, 8)), jnp.float32),
        "weight": normal_values(key_of[3], (ROWS, COLS), 1.0, 6.0, ((0, 4), (1, 8)), jnp.float32),
        "norm_scale": jnp.clip(jnp.exp(jax.random.uniform(key_of[4], (), jnp.float32, math.log(128.99231), math.log(257.98462))), 128.99231, 257.98462),
        "step_size": jnp.clip(jnp.exp(jax.random.uniform(key_of[5], (), jnp.float32, math.log(0.5), math.log(2.0))), 0.5, 2.0),
    }


def reference(activations, out_grad, momentum, weight, norm_scale, step_size):
    gradient = jnp.dot(activations.T, out_grad, preferred_element_type=jnp.float32)
    new_momentum = 0.95 * momentum + gradient
    scaled = (new_momentum / norm_scale).astype(jnp.bfloat16)
    gram = jnp.dot(scaled.T, scaled, preferred_element_type=jnp.float32).astype(jnp.bfloat16)
    first_power = jnp.dot(scaled, gram, preferred_element_type=jnp.float32).astype(jnp.bfloat16)
    second_power = jnp.dot(first_power, gram, preferred_element_type=jnp.float32)
    direction = 3.4445 * scaled.astype(jnp.float32) - 4.775 * first_power.astype(jnp.float32) + 2.0315 * second_power
    factor = 0.2 * math.sqrt(max(ROWS, COLS))
    new_weight = weight - step_size * factor * direction
    return (new_weight, new_momentum)
```

```python
import functools
import math

import jax
import jax.numpy as jnp
from jax import lax
from jax.experimental import pallas as pl
from jax.experimental.pallas import tpu as pltpu
from jax.sharding import PartitionSpec as P

ROWS = 4224
COLS = 4096
MESH = pl.DeviceIdType.MESH


def inner_rows(left, right):
    return lax.dot_general(
        left, right, (((0,), (0,)), ((), ())), preferred_element_type=jnp.float32
    )


def step_kernel(
    n, groups, factor,
    act_ref, grad_ref, momentum_hbm, weight_hbm, scale_ref, step_ref,
    new_weight_hbm, new_momentum_hbm,
    line, tiles, grads, panel, powers, gram, parts, from_core, from_chip,
    momentum, weight, total,
    z_send, z_recv, t_send, t_recv, g_send, g_recv,
    x_send, x_recv, y_send, y_recv, c_send, c_recv, p_send, p_recv, s_send, s_recv,
    load_sem, store_sem,
):
    half = act_ref.shape[0]
    rows, width = momentum.shape
    wide, middle, layers = width // 2, n // 2, n // 2
    core_rows, share = wide // 2, wide // groups
    row_tile = half // 3 if half % 48 == 0 else half
    a, b = lax.axis_index("aa"), lax.axis_index("ba")
    x, c, z, y = a // 2, a % 2, b // 2, b % 2
    core_mate = 2 * x + 1 - c
    chip_mate = 2 * (1 - x) + c
    y_mate = 2 * z + 1 - y

    loads = [
        pltpu.make_async_copy(momentum_hbm, momentum, load_sem.at[0]),
        pltpu.make_async_copy(weight_hbm, weight, load_sem.at[1]),
    ]
    for load in loads:
        load.start()

    place = z + y * (n - 1 - 2 * z)

    def at(position):
        position = (position + n) % n
        column = position // middle
        return 2 * (position + column * (n - 1 - 2 * position)) + column

    neighbours = (at(place + 1), at(place - 1))

    barrier = pltpu.get_barrier_semaphore()
    for r in range(1, groups):
        pl.semaphore_signal(barrier, 1, device_id={"aa": (a + r) % groups}, device_id_type=MESH)
    for r in range(groups):
        pl.semaphore_signal(
            barrier, 1, device_id={"aa": (a + r) % groups, "ba": y_mate}, device_id_type=MESH
        )

    @pl.when(z > 0)
    def _():
        pl.semaphore_signal(barrier, 1, device_id={"ba": b - 2}, device_id_type=MESH)

    @pl.when(z < layers - 1)
    def _():
        pl.semaphore_signal(barrier, 1, device_id={"ba": b + 2}, device_id_type=MESH)

    sides = (z + layers - 1) // layers + (2 * layers - 2 - z) // layers
    pl.semaphore_wait(barrier, 2 * groups - 1 + sides)

    def z_hop(source, layer, side):
        return pltpu.make_async_remote_copy(
            src_ref=source, dst_ref=line.at[layer],
            send_sem=z_send.at[side, layer], recv_sem=z_recv.at[layer],
            device_id={"ba": b + 2 - 4 * side}, device_id_type=MESH,
        )

    def near_copy(source, layer):
        return pltpu.make_async_remote_copy(
            src_ref=source, dst_ref=tiles.at[y, a],
            send_sem=t_send.at[0, layer], recv_sem=t_recv.at[y, a],
            device_id={"aa": layer}, device_id_type=MESH,
        )

    def far_copy(source, layer):
        return pltpu.make_async_remote_copy(
            src_ref=source, dst_ref=tiles.at[y, a],
            send_sem=t_send.at[1, layer], recv_sem=t_recv.at[y, a],
            device_id={"aa": layer, "ba": y_mate}, device_id_type=MESH,
        )

    def deliver(source, layer):
        far_copy(source, layer).start()

        @pl.when(layer != a)
        def _():
            near_copy(source, layer).start()

        @pl.when(layer == a)
        def _():
            tiles[y, a] = source[...]

    def grad_copy(kind):
        mate = chip_mate if kind == 0 else core_mate
        source, slot = (grads.at[chip_mate], chip_mate) if kind == 2 else (grad_ref, a)
        return pltpu.make_async_remote_copy(
            src_ref=source, dst_ref=grads.at[slot],
            send_sem=g_send.at[kind], recv_sem=g_recv.at[kind],
            device_id={"aa": mate}, device_id_type=MESH,
        )

    can_go = (z < layers - 1, z > 0)
    for side in range(2):
        pl.when(can_go[side])(z_hop(act_ref, z, side).start)
    grad_copy(0).start()
    grad_copy(1).start()
    deliver(act_ref, z)
    grads[a] = grad_ref[...]
    for distance in range(1, layers):
        for side in range(2):
            layer = z - distance if side == 0 else z + distance

            @pl.when((layer >= 0) & (layer < layers))
            def _():
                z_hop(line.at[layer], layer, side).wait_recv()
                pl.when(can_go[side])(z_hop(line.at[layer], layer, side).start)
                deliver(line.at[layer], layer)

        if distance == 1:
            grad_copy(0).wait_recv()
            grad_copy(2).start()
    grad_copy(1).wait_recv()
    grad_copy(2).wait_recv()
    for load in loads:
        load.wait()

    order = [(h, k) for k in range(2) for h in range(2)]

    def hop(held, send, recv, d, s, h, k):
        target = n - 1 if s == middle else 2 * s - 1 + d
        origin = 0 if s == 1 else 2 * s - 3 + d
        part = pl.ds(k * half, half)
        return pltpu.make_async_remote_copy(
            src_ref=held.at[origin, h, part], dst_ref=held.at[target, h, part],
            send_sem=send.at[d, s - 1, h, k], recv_sem=recv.at[d, s - 1, h, k],
            device_id={"ba": neighbours[d]}, device_id_type=MESH,
        )

    def goes(by_rows, d, s, h, k):
        return s < middle or d == (k if by_rows else h)

    def pass_on(held, send, recv, by_rows, d, s, h, k):
        hop(held, send, recv, d, s, h, k).wait_recv()
        if s < middle and goes(by_rows, d, s + 1, h, k):
            hop(held, send, recv, d, s + 1, h, k).start()

    def drain(held, send, recv, by_rows):
        for s in range(1, middle + 1):
            for h, k in order:
                for d in range(2):
                    if goes(by_rows, d, s, h, k):
                        hop(held, send, recv, d, s, h, k).wait_send()

    for k in range(2):
        for r in range(groups):
            pl.when((k != y) | (r != a))(
                pltpu.make_async_remote_copy(
                    src_ref=act_ref, dst_ref=tiles.at[k, r],
                    send_sem=t_send.at[0, 0], recv_sem=t_recv.at[k, r],
                    device_id={"aa": core_mate}, device_id_type=MESH,
                ).wait_recv
            )

        @pl.loop(0, half // row_tile)
        def _(t):
            source = pl.ds(pl.multiple_of(t * row_tile, 16), row_tile)
            part = pl.ds(pl.multiple_of(k * half + t * row_tile, 16), row_tile)
            gradient = sum(
                jnp.dot(tiles[k, r, source, :], grads[r], preferred_element_type=jnp.float32)
                for r in range(groups)
            )
            updated = 0.95 * momentum[part, :] + gradient
            momentum[part, :] = updated
            scaled = (updated / scale_ref[0]).astype(jnp.bfloat16)
            for h in range(2):
                panel[0, h, part, :] = scaled[:, h * wide : (h + 1) * wide]

        for h in range(2):
            for d in range(2):
                hop(panel, x_send, x_recv, d, 1, h, k).start()

    store_momentum = pltpu.make_async_copy(momentum, new_momentum_hbm, store_sem.at[0])
    store_momentum.start()

    def to_mate(source, target, send, recv, mate):
        return pltpu.make_async_remote_copy(
            src_ref=source, dst_ref=target, send_sem=send, recv_sem=recv,
            device_id={"aa": mate}, device_id_type=MESH,
        )

    def span(start, size):
        return pl.ds(pl.multiple_of(start, size), size)

    mine, theirs = c * core_rows + x * share, c * core_rows + (1 - x) * share

    def core_copy(e, h):
        return to_mate(
            parts.at[e, h, span((1 - c) * core_rows, core_rows)], from_core.at[e, h],
            c_send.at[e, h], c_recv.at[e, h], core_mate,
        )

    def chip_copy(e, h):
        return to_mate(
            parts.at[e, h, span(theirs, share)], from_chip.at[e, h],
            p_send.at[e, h], p_recv.at[e, h], chip_mate,
        )

    def share_copy(e, h, step):
        rows_of = gram.at[e, span(h * wide + (theirs if step == 2 else mine), share)]
        return to_mate(
            rows_of, rows_of, s_send.at[e, h, step], s_recv.at[e, h, step],
            chip_mate if step == 0 else core_mate,
        )

    def gram_partial(e, h):
        @pl.loop(0, 2)
        def _(q):
            parts[e, h, :, span(q * wide, wide)] = inner_rows(panel[e, h], panel[0, q])

        core_copy(e, h).start()

    def core_sum(e, h):
        core_copy(e, h).wait_recv()
        parts[e, h, span(theirs, share)] += from_core[e, h, span((1 - x) * share, share)]
        chip_copy(e, h).start()
        parts[e, h, span(mine, share)] += from_core[e, h, span(x * share, share)]

    def gram_share(e, h):
        chip_copy(e, h).wait_recv()
        gram[e, span(h * wide + mine, share)] = (
            parts[e, h, span(mine, share)] + from_chip[e, h]
        ).astype(jnp.bfloat16)
        share_copy(e, h, 0).start()
        share_copy(e, h, 1).start()

    def relay(e, h):
        share_copy(e, h, 0).wait_recv()
        share_copy(e, h, 2).start()

    def gram_ready(e, h):
        share_copy(e, h, 1).wait_recv()
        share_copy(e, h, 2).wait_recv()

    def accumulate(held, e, halves, first, start, count):
        @pl.loop(0, count // row_tile)
        def _(t):
            part = pl.ds(pl.multiple_of(start + t * row_tile, 16), row_tile)
            term = sum(
                jnp.dot(
                    held[e, h, part, :], gram[e, h * wide : (h + 1) * wide, :],
                    preferred_element_type=jnp.float32,
                )
                for h in halves
            )
            if first:
                total[part, :] = term
            else:
                total[part, :] += term

    summed, shared = [], []

    def advance():
        for unit in shared:
            relay(*unit)
        for unit in summed:
            gram_share(*unit)
        shared[:] = summed
        summed[:] = []

    def use_units(units):
        for unit in units:
            gram_partial(*unit)
        advance()
        for unit in units:
            core_sum(*unit)
        summed[:] = units

    ring_x = (panel, x_send, x_recv, True)
    use_units([(0, 0), (0, 1)])
    for s in range(1, middle):
        for i, (h, k) in enumerate(order):
            for d in range(2):
                pass_on(*ring_x, d, s, h, k)
            if i == 1:
                advance()
        use_units([(e, h) for h in range(2) for e in (2 * s - 1, 2 * s)])
    last = n - 1
    for h in range(2):
        for d in range(2):
            pass_on(*ring_x, d, middle, h, d)
        if h == 0:
            use_units([(last, 0)])
    gram_partial(last, 1)
    advance()
    for e in range(n):
        if e == 1:
            core_sum(last, 1)
        if e == 3:
            advance()
            summed[:] = [(last, 1)]
        if e == last - 2:
            advance()
        if e == last:
            advance()
        for h in range(2 if e < last else 1):
            gram_ready(e, h)
        accumulate(panel, e, (0, 1) if e < last else (0,), e == 0, 0, rows)
    advance()
    gram_ready(last, 1)

    ring_p = (powers, y_send, y_recv, False)
    for k in range(2):
        part = pl.ds(k * half, half)
        accumulate(panel, last, (1,), False, k * half, half)
        for h in range(2):
            powers[0, h, part, :] = total[part, h * wide : (h + 1) * wide].astype(jnp.bfloat16)
            for d in range(2):
                hop(powers, y_send, y_recv, d, 1, h, k).start()

    accumulate(powers, 0, (0, 1), True, 0, rows)
    for s in range(1, middle):
        for h, k in order:
            for d in range(2):
                pass_on(*ring_p, d, s, h, k)
        for e in (2 * s - 1, 2 * s):
            accumulate(powers, e, (0, 1), False, 0, rows)

    rate = step_ref[0] * factor
    stores = []
    for k in range(2):
        for d in range(2):
            pass_on(*ring_p, d, middle, d, k)
        accumulate(powers, last, (0, 1), False, k * half, half)
        part = pl.ds(k * half, half)
        for h in range(2):
            columns = slice(h * wide, (h + 1) * wide)
            direction = (
                3.4445 * panel[0, h, part, :].astype(jnp.float32)
                - 4.775 * powers[0, h, part, :].astype(jnp.float32)
                + 2.0315 * total[part, columns]
            )
            weight[part, columns] = weight[part, columns] - rate * direction
        stores.append(
            pltpu.make_async_copy(
                weight.at[part], new_weight_hbm.at[part], store_sem.at[1 + k]
            )
        )
        stores[-1].start()

    drain(*ring_x)
    drain(*ring_p)
    for e in range(n):
        for h in range(2):
            core_copy(e, h).wait_send()
            chip_copy(e, h).wait_send()
            for step in range(3):
                share_copy(e, h, step).wait_send()
    for kind in range(3):
        grad_copy(kind).wait_send()
    for layer in range(layers):
        far_copy(act_ref, layer).wait_send()
        pl.when(layer != a)(near_copy(act_ref, layer).wait_send)
        for side in range(2):
            from_here = layer <= z if side == 0 else layer >= z
            pl.when(from_here & can_go[side])(z_hop(act_ref, layer, side).wait_send)
    store_momentum.wait()
    for store in stores:
        store.wait()


def fused_step(activations, out_grad, momentum, weight, norm_scale, step_size, n, groups):
    tokens, features = activations.shape
    rows, width = momentum.shape
    wide, middle = width // 2, n // 2
    dma = pltpu.SemaphoreType.DMA
    vmem = pl.BlockSpec(memory_space=pltpu.VMEM)
    hbm = pl.BlockSpec(memory_space=pl.ANY)
    smem = pl.BlockSpec(memory_space=pltpu.SMEM)
    ring = dma((2, middle, 2, 2))
    units = dma((n, 2))
    return pl.pallas_call(
        functools.partial(step_kernel, n, groups, 0.2 * math.sqrt(max(ROWS, COLS))),
        out_shape=(
            jax.ShapeDtypeStruct((rows, width), jnp.float32),
            jax.ShapeDtypeStruct((rows, width), jnp.float32),
        ),
        in_specs=[vmem, vmem, hbm, hbm, smem, smem],
        out_specs=(hbm, hbm),
        scratch_shapes=[
            pltpu.VMEM((n // 2, features, tokens), jnp.bfloat16),
            pltpu.VMEM((2, groups, features, tokens), jnp.bfloat16),
            pltpu.VMEM((groups, tokens, width), jnp.bfloat16),
            pltpu.VMEM((n, 2, rows, wide), jnp.bfloat16),
            pltpu.VMEM((n, 2, rows, wide), jnp.bfloat16),
            pltpu.VMEM((n, width, width), jnp.bfloat16),
            pltpu.VMEM((n, 2, wide, width), jnp.float32),
            pltpu.VMEM((n, 2, wide // 2, width), jnp.float32),
            pltpu.VMEM((n, 2, wide // groups, width), jnp.float32),
            pltpu.VMEM((rows, width), jnp.float32),
            pltpu.VMEM((rows, width), jnp.float32),
            pltpu.VMEM((rows, width), jnp.float32),
            dma((2, n // 2)), dma((n // 2,)),
            dma((2, n // 2)), dma((2, groups)),
            dma((3,)), dma((3,)),
            ring, ring, ring, ring,
            units, units, units, units,
            dma((n, 2, 3)), dma((n, 2, 3)),
            dma((2,)), dma((3,)),
        ],
        compiler_params=pltpu.CompilerParams(
            collective_id=0, has_side_effects=True, vmem_limit_bytes=62 * 1024 * 1024
        ),
        name="step",
    )(activations.T, out_grad, momentum, weight, norm_scale.reshape(1), step_size.reshape(1))


def plain_gradient(activations, out_grad):
    features = lax.all_to_all(
        lax.all_gather(activations, "ba", axis=1, tiled=True),
        "aa", split_axis=1, concat_axis=0, tiled=True,
    )
    return inner_rows(features, lax.all_gather(out_grad, "aa", axis=0, tiled=True))


def plain_direction(scaled):
    row_panel = lax.all_gather(scaled, "ba", axis=1, tiled=True)
    gram_part = inner_rows(row_panel, scaled)
    width = gram_part.shape[0]
    groups = lax.axis_size("aa")
    padding = (groups - width % groups) % groups
    padded = jnp.pad(gram_part, ((0, padding), (0, 0)))
    share = lax.psum_scatter(padded, "aa", scatter_dimension=0, tiled=True).astype(jnp.bfloat16)
    gram_cols = lax.all_gather(share, "aa", axis=0, tiled=True)[:width]
    first_power = jnp.dot(row_panel, gram_cols, preferred_element_type=jnp.float32).astype(
        jnp.bfloat16
    )
    second_power = jnp.dot(
        lax.all_gather(first_power, "ba", axis=1, tiled=True),
        gram_cols,
        preferred_element_type=jnp.float32,
    )
    return (
        3.4445 * scaled.astype(jnp.float32)
        - 4.775 * first_power.astype(jnp.float32)
        + 2.0315 * second_power
    )


def per_device(activations, out_grad, momentum, weight, norm_scale, step_size):
    n, groups = lax.axis_size("ba"), lax.axis_size("aa")
    rows, width = momentum.shape
    tokens, features = activations.shape
    fits = (
        groups == 4 and n == 2 * groups and rows == 2 * features
        and features % 16 == 0 and tokens % 128 == 0 and width % 256 == 0
        and width % (32 * groups) == 0
        and 4 * n * rows * width + 9 * n * width * width + 17 * rows * width < 56 * 2**20
    )
    if fits:
        return fused_step(
            activations, out_grad, momentum, weight, norm_scale, step_size, n, groups
        )
    new_momentum = 0.95 * momentum + plain_gradient(activations, out_grad)
    scaled = (new_momentum / norm_scale).astype(jnp.bfloat16)
    factor = 0.2 * math.sqrt(max(ROWS, COLS))
    new_weight = weight - step_size * factor * plain_direction(scaled)
    return (new_weight, new_momentum)


def solution(mesh):
    placed = (P("aa", "ba"), P("aa", "ba"), P("aa", "ba"), P("aa", "ba"), P(), P())
    return jax.shard_map(
        per_device,
        mesh=mesh,
        in_specs=placed,
        out_specs=(P("aa", "ba"), P("aa", "ba")),
        check_vma=False,
    )
```

```python
import functools
import math

import jax
import jax.numpy as jnp
from jax import lax
from jax.experimental import pallas as pl
from jax.experimental.pallas import tpu as pltpu
from jax.sharding import PartitionSpec as P

ROWS = 4224
COLS = 4096
MESH = pl.DeviceIdType.MESH


def inner_rows(left, right):
    return lax.dot_general(
        left, right, (((0,), (0,)), ((), ())), preferred_element_type=jnp.float32
    )


def step_kernel(
    n, groups, factor,
    act_ref, grad_ref, momentum_hbm, weight_hbm, scale_ref, step_ref,
    weight, momentum,
    line, tiles, grads, panel, powers, gram, parts, from_core, from_chip, total,
    z_send, z_recv, t_send, t_recv, r_send, g_send, g_recv,
    x_send, x_recv, y_send, y_recv, c_send, c_recv, p_send, p_recv, s_send, s_recv,
    load_sem,
):
    half = act_ref.shape[0]
    rows, width = momentum.shape
    wide, middle, layers = width // 2, n // 2, n // 2
    core_rows, share = wide // 2, wide // groups
    pieces = 3 if half % 48 == 0 else 1
    a, b = lax.axis_index("aa"), lax.axis_index("ba")
    x, c, z, y = a // 2, a % 2, b // 2, b % 2
    core_mate = 2 * x + 1 - c
    chip_mate = 2 * (1 - x) + c
    y_mate = 2 * z + 1 - y

    loads = [
        pltpu.make_async_copy(momentum_hbm, momentum, load_sem.at[0]),
        pltpu.make_async_copy(weight_hbm, weight, load_sem.at[1]),
    ]
    for load in loads:
        load.start()

    place = z + y * (n - 1 - 2 * z)

    def at(position):
        position = (position + n) % n
        column = position // middle
        return 2 * (position + column * (n - 1 - 2 * position)) + column

    neighbours = (at(place + 1), at(place - 1))

    barrier = pltpu.get_barrier_semaphore()
    for r in range(1, groups):
        pl.semaphore_signal(barrier, 1, device_id={"aa": (a + r) % groups}, device_id_type=MESH)
    for r in range(groups):
        pl.semaphore_signal(
            barrier, 1, device_id={"aa": (a + r) % groups, "ba": y_mate}, device_id_type=MESH
        )

    @pl.when(z > 0)
    def _():
        pl.semaphore_signal(barrier, 1, device_id={"ba": b - 2}, device_id_type=MESH)

    @pl.when(z < layers - 1)
    def _():
        pl.semaphore_signal(barrier, 1, device_id={"ba": b + 2}, device_id_type=MESH)

    sides = (z + layers - 1) // layers + (2 * layers - 2 - z) // layers
    pl.semaphore_wait(barrier, 2 * groups - 1 + sides)

    piece = half // pieces

    def cut(j):
        return pl.ds(j * piece, piece)

    def z_hop(source, layer, side, j):
        return pltpu.make_async_remote_copy(
            src_ref=source.at[cut(j)], dst_ref=line.at[layer, cut(j)],
            send_sem=z_send.at[side, layer, j], recv_sem=z_recv.at[layer, j],
            device_id={"ba": b + 2 - 4 * side}, device_id_type=MESH,
        )

    def near_copy(source, layer, j):
        return pltpu.make_async_remote_copy(
            src_ref=source.at[cut(j)], dst_ref=tiles.at[y, a, cut(j)],
            send_sem=t_send.at[0, layer, j], recv_sem=t_recv.at[y, a, j],
            device_id={"aa": layer}, device_id_type=MESH,
        )

    def far_copy(source, layer, j):
        return pltpu.make_async_remote_copy(
            src_ref=source.at[cut(j)], dst_ref=tiles.at[y, a, cut(j)],
            send_sem=t_send.at[1, layer, j], recv_sem=t_recv.at[y, a, j],
            device_id={"aa": layer, "ba": y_mate}, device_id_type=MESH,
        )

    def relay_copy(q, j):
        origin = 2 * (1 - x) + q
        return pltpu.make_async_remote_copy(
            src_ref=tiles.at[y, origin, cut(j)], dst_ref=tiles.at[y, origin, cut(j)],
            send_sem=r_send.at[q, j], recv_sem=t_recv.at[y, origin, j],
            device_id={"ba": y_mate}, device_id_type=MESH,
        )

    def tile_arrival(k, r, j):
        return pltpu.make_async_remote_copy(
            src_ref=act_ref.at[cut(j)], dst_ref=tiles.at[k, r, cut(j)],
            send_sem=t_send.at[0, 0, j], recv_sem=t_recv.at[k, r, j],
            device_id={"aa": core_mate}, device_id_type=MESH,
        )

    def deliver(source, layer, j):
        pl.when(layer // 2 == x)(far_copy(source, layer, j).start)
        pl.when(layer != a)(near_copy(source, layer, j).start)

        @pl.when(layer == a)
        def _():
            tiles[y, a, cut(j)] = source[cut(j)]

    def grad_copy(kind):
        mate = chip_mate if kind == 0 else core_mate
        source, slot = (grads.at[chip_mate], chip_mate) if kind == 2 else (grad_ref, a)
        return pltpu.make_async_remote_copy(
            src_ref=source, dst_ref=grads.at[slot],
            send_sem=g_send.at[kind], recv_sem=g_recv.at[kind],
            device_id={"aa": mate}, device_id_type=MESH,
        )

    can_go = (z < layers - 1, z > 0)
    for j in range(pieces):
        for side in range(2):
            pl.when(can_go[side])(z_hop(act_ref, z, side, j).start)
        deliver(act_ref, z, j)
        if j == 0:
            grad_copy(0).start()
            grad_copy(1).start()
    grads[a] = grad_ref[...]
    for distance in range(1, layers + 1):
        if distance < layers:
            for j in range(pieces):
                for side in range(2):
                    layer = z - distance if side == 0 else z + distance

                    @pl.when((layer >= 0) & (layer < layers))
                    def _():
                        z_hop(line.at[layer], layer, side, j).wait_recv()
                        pl.when(can_go[side])(z_hop(line.at[layer], layer, side, j).start)
                        deliver(line.at[layer], layer, j)

        @pl.when((z - a == distance - 1) | (a - z == distance - 1))
        def _():
            for j in range(pieces):
                for q in range(2):
                    tile_arrival(y, 2 * (1 - x) + q, j).wait_recv()
                    relay_copy(q, j).start()

        if distance == 1:
            grad_copy(0).wait_recv()
            grad_copy(2).start()
    grad_copy(1).wait_recv()
    grad_copy(2).wait_recv()
    for load in loads:
        load.wait()

    by_columns = [(h, k) for h in range(2) for k in range(2)]
    by_halves = [(h, k) for k in range(2) for h in range(2)]

    def hop(held, send, recv, d, s, h, k):
        target = n - 1 if s == middle else 2 * s - 1 + d
        origin = 0 if s == 1 else 2 * s - 3 + d
        part = pl.ds(k * half, half)
        return pltpu.make_async_remote_copy(
            src_ref=held.at[origin, h, part], dst_ref=held.at[target, h, part],
            send_sem=send.at[d, s - 1, h, k], recv_sem=recv.at[d, s - 1, h, k],
            device_id={"ba": neighbours[d]}, device_id_type=MESH,
        )

    def goes(first, d, s, h, k):
        return s < middle or d == (k if first else h)

    def pass_on(held, send, recv, first, d, s, h, k):
        hop(held, send, recv, d, s, h, k).wait_recv()
        if s < middle and goes(first, d, s + 1, h, k):
            hop(held, send, recv, d, s + 1, h, k).start()

    def drain(held, send, recv, first):
        for s in range(1, middle + 1):
            for h, k in by_columns:
                for d in range(2):
                    if goes(first, d, s, h, k):
                        hop(held, send, recv, d, s, h, k).wait_send()

    for k in range(2):
        for r in range(groups):
            @pl.when((k != y) | ((r // 2 == x) & (r != a)))
            def _():
                for j in range(pieces):
                    tile_arrival(k, r, j).wait_recv()

        @pl.loop(0, pieces)
        def _(t):
            source = pl.ds(pl.multiple_of(t * piece, 16), piece)
            part = pl.ds(pl.multiple_of(k * half + t * piece, 16), piece)
            gradient = sum(
                jnp.dot(tiles[k, r, source, :], grads[r], preferred_element_type=jnp.float32)
                for r in range(groups)
            )
            updated = 0.95 * momentum[part, :] + gradient
            momentum[part, :] = updated
            scaled = (updated / scale_ref[0]).astype(jnp.bfloat16)
            for h in range(2):
                panel[0, h, part, :] = scaled[:, h * wide : (h + 1) * wide]

    for h, k in by_columns:
        for d in range(2):
            hop(panel, x_send, x_recv, d, 1, h, k).start()

    def to_mate(source, target, send, recv, mate):
        return pltpu.make_async_remote_copy(
            src_ref=source, dst_ref=target, send_sem=send, recv_sem=recv,
            device_id={"aa": mate}, device_id_type=MESH,
        )

    def span(start, size):
        return pl.ds(pl.multiple_of(start, size), size)

    mine, theirs = c * core_rows + x * share, c * core_rows + (1 - x) * share

    def core_copy(e, h):
        return to_mate(
            parts.at[e, h, span((1 - c) * core_rows, core_rows)], from_core.at[e, h],
            c_send.at[e, h], c_recv.at[e, h], core_mate,
        )

    def chip_copy(e, h):
        return to_mate(
            parts.at[e, h, span(theirs, share)], from_chip.at[e, h],
            p_send.at[e, h], p_recv.at[e, h], chip_mate,
        )

    def share_copy(e, h, step):
        rows_of = gram.at[e, span(h * wide + (theirs if step == 2 else mine), share)]
        return to_mate(
            rows_of, rows_of, s_send.at[e, h, step], s_recv.at[e, h, step],
            chip_mate if step == 0 else core_mate,
        )

    def gram_partial(e, h):
        @pl.loop(0, 2)
        def _(q):
            parts[e, h, :, span(q * wide, wide)] = inner_rows(panel[e, h], panel[0, q])

        core_copy(e, h).start()

    def core_sum(e, h):
        core_copy(e, h).wait_recv()
        parts[e, h, span(theirs, share)] += from_core[e, h, span((1 - x) * share, share)]
        chip_copy(e, h).start()
        parts[e, h, span(mine, share)] += from_core[e, h, span(x * share, share)]

    def gram_share(e, h):
        chip_copy(e, h).wait_recv()
        gram[e, span(h * wide + mine, share)] = (
            parts[e, h, span(mine, share)] + from_chip[e, h]
        ).astype(jnp.bfloat16)
        share_copy(e, h, 0).start()
        share_copy(e, h, 1).start()

    def relay(e, h):
        share_copy(e, h, 0).wait_recv()
        share_copy(e, h, 2).start()

    def gram_ready(e, h):
        share_copy(e, h, 1).wait_recv()
        share_copy(e, h, 2).wait_recv()

    def accumulate(held, e, halves, first, start, count):
        @pl.loop(0, count // half)
        def _(t):
            part = pl.ds(pl.multiple_of(start + t * half, 16), half)
            term = sum(
                jnp.dot(
                    held[e, h, part, :], gram[e, h * wide : (h + 1) * wide, :],
                    preferred_element_type=jnp.float32,
                )
                for h in halves
            )
            if first:
                total[part, :] = term
            else:
                total[part, :] += term

    ring_x = (panel, x_send, x_recv, True)
    steps = [[(0, 0), (0, 1)]]
    for unit in steps[0]:
        gram_partial(*unit)
    for s in range(1, middle + 1):
        for h in range(2):
            for k in range(2):
                for d in range(2):
                    if goes(True, d, s, h, k):
                        pass_on(*ring_x, d, s, h, k)
            if len(steps) == 1:
                for unit in steps[0]:
                    core_sum(*unit)
            units = [(2 * s - 1, h), (2 * s, h)] if s < middle else [(n - 1, h)]
            for unit in units:
                gram_partial(*unit)
            if len(steps) > 1:
                for unit in steps[-2]:
                    relay(*unit)
            if (s, h) != (middle, 1):
                for unit in steps[-1]:
                    gram_share(*unit)
                for unit in units:
                    core_sum(*unit)
            steps.append(units)
    last = n - 1
    for e in range(n):
        if e == 1:
            core_sum(last, 1)
            gram_share(last, 0)
        if e == last - 2:
            relay(last, 0)
        if e == last - 1:
            gram_share(last, 1)
        for h in range(2 if e < last else 1):
            gram_ready(e, h)
        accumulate(panel, e, (0, 1) if e < last else (0,), e == 0, 0, rows)
    relay(last, 1)
    gram_ready(last, 1)

    ring_p = (powers, y_send, y_recv, False)
    for k in range(2):
        part = pl.ds(k * half, half)
        accumulate(panel, last, (1,), False, k * half, half)
        for h in range(2):
            powers[0, h, part, :] = total[part, h * wide : (h + 1) * wide].astype(jnp.bfloat16)
            for d in range(2):
                hop(powers, y_send, y_recv, d, 1, h, k).start()

    accumulate(powers, 0, (0, 1), True, 0, rows)
    for s in range(1, middle):
        for h, k in by_halves:
            for d in range(2):
                pass_on(*ring_p, d, s, h, k)
        for e in (2 * s - 1, 2 * s):
            accumulate(powers, e, (0, 1), False, 0, rows)

    rate = step_ref[0] * factor
    for k in range(2):
        for d in range(2):
            pass_on(*ring_p, d, middle, d, k)
        accumulate(powers, last, (0, 1), False, k * half, half)
        part = pl.ds(k * half, half)
        for h in range(2):
            columns = slice(h * wide, (h + 1) * wide)
            direction = (
                3.4445 * panel[0, h, part, :].astype(jnp.float32)
                - 4.775 * powers[0, h, part, :].astype(jnp.float32)
                + 2.0315 * total[part, columns]
            )
            weight[part, columns] = weight[part, columns] - rate * direction

    drain(*ring_x)
    drain(*ring_p)
    for e in range(n):
        for h in range(2):
            core_copy(e, h).wait_send()
            chip_copy(e, h).wait_send()
            for step in range(3):
                share_copy(e, h, step).wait_send()
    for kind in range(3):
        grad_copy(kind).wait_send()
    for j in range(pieces):
        for q in range(2):
            relay_copy(q, j).wait_send()
        for layer in range(layers):
            pl.when(layer // 2 == x)(far_copy(act_ref, layer, j).wait_send)
            pl.when(layer != a)(near_copy(act_ref, layer, j).wait_send)
            for side in range(2):
                from_here = layer <= z if side == 0 else layer >= z
                pl.when(from_here & can_go[side])(z_hop(act_ref, layer, side, j).wait_send)


def fused_step(activations, out_grad, momentum, weight, norm_scale, step_size, n, groups):
    tokens, features = activations.shape
    rows, width = momentum.shape
    wide, middle = width // 2, n // 2
    pieces = 3 if features % 48 == 0 else 1
    dma = pltpu.SemaphoreType.DMA
    vmem = pl.BlockSpec(memory_space=pltpu.VMEM)
    hbm = pl.BlockSpec(memory_space=pl.ANY)
    smem = pl.BlockSpec(memory_space=pltpu.SMEM)
    ring = dma((2, middle, 2, 2))
    units = dma((n, 2))
    return pl.pallas_call(
        functools.partial(step_kernel, n, groups, 0.2 * math.sqrt(max(ROWS, COLS))),
        out_shape=(
            jax.ShapeDtypeStruct((rows, width), jnp.float32),
            jax.ShapeDtypeStruct((rows, width), jnp.float32),
        ),
        in_specs=[vmem, vmem, hbm, hbm, smem, smem],
        out_specs=(vmem, vmem),
        scratch_shapes=[
            pltpu.VMEM((n // 2, features, tokens), jnp.bfloat16),
            pltpu.VMEM((2, groups, features, tokens), jnp.bfloat16),
            pltpu.VMEM((groups, tokens, width), jnp.bfloat16),
            pltpu.VMEM((n, 2, rows, wide), jnp.bfloat16),
            pltpu.VMEM((n, 2, rows, wide), jnp.bfloat16),
            pltpu.VMEM((n, width, width), jnp.bfloat16),
            pltpu.VMEM((n, 2, wide, width), jnp.float32),
            pltpu.VMEM((n, 2, wide // 2, width), jnp.float32),
            pltpu.VMEM((n, 2, wide // groups, width), jnp.float32),
            pltpu.VMEM((rows, width), jnp.float32),
            dma((2, n // 2, pieces)), dma((n // 2, pieces)),
            dma((2, n // 2, pieces)), dma((2, groups, pieces)), dma((2, pieces)),
            dma((3,)), dma((3,)),
            ring, ring, ring, ring,
            units, units, units, units,
            dma((n, 2, 3)), dma((n, 2, 3)),
            dma((2,)),
        ],
        compiler_params=pltpu.CompilerParams(
            collective_id=0, has_side_effects=True, vmem_limit_bytes=48 * 1024 * 1024
        ),
        name="step",
    )(activations.T, out_grad, momentum, weight, norm_scale.reshape(1), step_size.reshape(1))


def plain_gradient(activations, out_grad):
    features = lax.all_to_all(
        lax.all_gather(activations, "ba", axis=1, tiled=True),
        "aa", split_axis=1, concat_axis=0, tiled=True,
    )
    return inner_rows(features, lax.all_gather(out_grad, "aa", axis=0, tiled=True))


def plain_direction(scaled):
    row_panel = lax.all_gather(scaled, "ba", axis=1, tiled=True)
    gram_part = inner_rows(row_panel, scaled)
    width = gram_part.shape[0]
    groups = lax.axis_size("aa")
    padding = (groups - width % groups) % groups
    padded = jnp.pad(gram_part, ((0, padding), (0, 0)))
    share = lax.psum_scatter(padded, "aa", scatter_dimension=0, tiled=True).astype(jnp.bfloat16)
    gram_cols = lax.all_gather(share, "aa", axis=0, tiled=True)[:width]
    first_power = jnp.dot(row_panel, gram_cols, preferred_element_type=jnp.float32).astype(
        jnp.bfloat16
    )
    second_power = jnp.dot(
        lax.all_gather(first_power, "ba", axis=1, tiled=True),
        gram_cols,
        preferred_element_type=jnp.float32,
    )
    return (
        3.4445 * scaled.astype(jnp.float32)
        - 4.775 * first_power.astype(jnp.float32)
        + 2.0315 * second_power
    )


def per_device(activations, out_grad, momentum, weight, norm_scale, step_size):
    n, groups = lax.axis_size("ba"), lax.axis_size("aa")
    rows, width = momentum.shape
    tokens, features = activations.shape
    fits = (
        groups == 4 and n == 2 * groups and rows == 2 * features
        and features % 16 == 0 and tokens % 128 == 0 and width % 256 == 0
        and width % (32 * groups) == 0
        and 4 * n * rows * width + 9 * n * width * width + 17 * rows * width < 56 * 2**20
    )
    if fits:
        return fused_step(
            activations, out_grad, momentum, weight, norm_scale, step_size, n, groups
        )
    new_momentum = 0.95 * momentum + plain_gradient(activations, out_grad)
    scaled = (new_momentum / norm_scale).astype(jnp.bfloat16)
    factor = 0.2 * math.sqrt(max(ROWS, COLS))
    new_weight = weight - step_size * factor * plain_direction(scaled)
    return (new_weight, new_momentum)


def solution(mesh):
    placed = (P("aa", "ba"), P("aa", "ba"), P("aa", "ba"), P("aa", "ba"), P(), P())
    return jax.shard_map(
        per_device,
        mesh=mesh,
        in_specs=placed,
        out_specs=(P("aa", "ba"), P("aa", "ba")),
        check_vma=False,
    )
```

```python
import functools
import math

import jax
import jax.numpy as jnp
from jax import lax
from jax.experimental import pallas as pl
from jax.experimental.pallas import tpu as pltpu
from jax.sharding import PartitionSpec as P

ROWS = 4224
COLS = 4096
MESH = pl.DeviceIdType.MESH


def inner_rows(left, right):
    return lax.dot_general(
        left, right, (((0,), (0,)), ((), ())), preferred_element_type=jnp.float32
    )


def step_kernel(
    n, groups, factor,
    act_hbm, grad_hbm, momentum_hbm, weight_hbm, scale_ref, step_ref,
    weight, momentum,
    line, stage, tiles, grads, panel, powers, gram, parts, from_core, from_chip, total,
    z_send, z_recv, t_send, t_recv, b_recv, g_send, g_recv,
    x_send, x_recv, y_send, y_recv, c_send, c_recv, p_send, p_recv, s_send, s_recv,
    load_sem,
):
    half = line.shape[1]
    rows, width = momentum.shape
    wide, middle, layers = width // 2, n // 2, n // 2
    core_rows, share = wide // 2, wide // groups
    pieces = 3 if half % 48 == 0 else 1
    a, b = lax.axis_index("aa"), lax.axis_index("ba")
    x, c, z, y = a // 2, a % 2, b // 2, b % 2
    core_mate = 2 * x + 1 - c
    chip_mate = 2 * (1 - x) + c
    y_mate = 2 * z + 1 - y

    loads = [
        pltpu.make_async_copy(act_hbm, line.at[z], load_sem.at[0]),
        pltpu.make_async_copy(grad_hbm, grads.at[a], load_sem.at[1]),
        pltpu.make_async_copy(momentum_hbm, momentum, load_sem.at[2]),
        pltpu.make_async_copy(weight_hbm, weight, load_sem.at[3]),
    ]
    for load in loads:
        load.start()

    place = z + y * (n - 1 - 2 * z)

    def at(position):
        position = (position + n) % n
        column = position // middle
        return 2 * (position + column * (n - 1 - 2 * position)) + column

    neighbours = (at(place + 1), at(place - 1))

    barrier = pltpu.get_barrier_semaphore()
    for r in range(1, groups):
        pl.semaphore_signal(barrier, 1, device_id={"aa": (a + r) % groups}, device_id_type=MESH)
    for r in range(groups):
        pl.semaphore_signal(
            barrier, 1, device_id={"aa": (a + r) % groups, "ba": y_mate}, device_id_type=MESH
        )

    @pl.when(z > 0)
    def _():
        pl.semaphore_signal(barrier, 1, device_id={"ba": b - 2}, device_id_type=MESH)

    @pl.when(z < layers - 1)
    def _():
        pl.semaphore_signal(barrier, 1, device_id={"ba": b + 2}, device_id_type=MESH)

    sides = (z + layers - 1) // layers + (2 * layers - 2 - z) // layers
    pl.semaphore_wait(barrier, 2 * groups - 1 + sides)

    piece = half // pieces

    def cut(j):
        return pl.ds(j * piece, piece)

    def remote(source, target, send, recv, where):
        return pltpu.make_async_remote_copy(
            src_ref=source, dst_ref=target, send_sem=send, recv_sem=recv,
            device_id=where, device_id_type=MESH,
        )

    def z_hop(layer, side, j):
        block = line.at[layer, cut(j)]
        return remote(
            block, block, z_send.at[side, layer], z_recv.at[layer, j], {"ba": b + 2 - 4 * side}
        )

    def near_copy(layer, j):
        return remote(
            line.at[layer, cut(j)], tiles.at[y, a, cut(j)], t_send.at[0], t_recv.at[y, a, j],
            {"aa": layer},
        )

    def far_copy(layer, j):
        return remote(
            line.at[layer, cut(j)], tiles.at[y, a, cut(j)], t_send.at[1], t_recv.at[y, a, j],
            {"aa": layer, "ba": y_mate},
        )

    def relay_copy(j):
        block = tiles.at[y, 2 * (1 - x), cut(j)]
        return remote(block, block, t_send.at[2], t_recv.at[y, 2 * (1 - x), j], {"ba": y_mate})

    def side_copy(layer, j):
        return remote(
            line.at[layer, cut(j)], stage.at[layer % 2, cut(j)], t_send.at[3],
            b_recv.at[layer % 2, j], {"ba": y_mate},
        )

    def cross_copy(slot, j):
        return remote(
            stage.at[slot, cut(j)], tiles.at[1 - y, a, cut(j)], t_send.at[4],
            t_recv.at[1 - y, a, j], {"aa": 2 * (1 - x) + slot},
        )

    def tile_arrival(k, r, j):
        block = tiles.at[k, r, cut(j)]
        return remote(block, block, t_send.at[0], t_recv.at[k, r, j], {"aa": core_mate})

    def deliver(layer, j):
        pl.when(layer // 2 == x)(far_copy(layer, j).start)
        pl.when((layer // 2 != x) & (c == 1))(side_copy(layer, j).start)
        pl.when(layer != a)(near_copy(layer, j).start)

        @pl.when(layer == a)
        def _():
            tiles[y, a, cut(j)] = line[layer, cut(j)]

    def grad_copy(kind):
        slot = chip_mate if kind == 2 else a
        return remote(
            grads.at[slot], grads.at[slot], g_send.at[kind], g_recv.at[kind],
            {"aa": chip_mate if kind == 0 else core_mate},
        )

    loads[0].wait()
    loads[1].wait()
    can_go = (z < layers - 1, z > 0)
    for j in range(pieces):
        for side in range(2):
            pl.when(can_go[side])(z_hop(z, side, j).start)
        deliver(z, j)
        if j == 0:
            grad_copy(0).start()
            grad_copy(1).start()
    for distance in range(1, layers + 1):
        if distance < layers:
            for j in range(pieces):
                for side in range(2):
                    layer = z - distance if side == 0 else z + distance

                    @pl.when((layer >= 0) & (layer < layers))
                    def _():
                        z_hop(layer, side, j).wait_recv()
                        pl.when(can_go[side])(z_hop(layer, side, j).start)
                        deliver(layer, j)

        for side in range(2):
            layer = z - distance + 1 if side == 0 else z + distance - 1
            there = (layer >= 0) & (layer < layers) & ((side == 0) | (distance > 1))

            @pl.when(there & (layer // 2 != x) & (c == 1))
            def _():
                for j in range(pieces):
                    side_copy(layer, j).wait_recv()
                    cross_copy(layer % 2, j).start()

        @pl.when((z - a == distance - 1) | (a - z == distance - 1))
        def _():
            for j in range(pieces):
                tile_arrival(y, 2 * (1 - x), j).wait_recv()
                relay_copy(j).start()

        if distance == 1:
            grad_copy(0).wait_recv()
            grad_copy(2).start()
    grad_copy(1).wait_recv()
    grad_copy(2).wait_recv()
    loads[2].wait()
    loads[3].wait()

    by_columns = [(h, k) for h in range(2) for k in range(2)]
    by_halves = [(h, k) for k in range(2) for h in range(2)]

    def hop(held, send, recv, d, s, h, k):
        target = n - 1 if s == middle else 2 * s - 1 + d
        origin = 0 if s == 1 else 2 * s - 3 + d
        part = pl.ds(k * half, half)
        return pltpu.make_async_remote_copy(
            src_ref=held.at[origin, h, part], dst_ref=held.at[target, h, part],
            send_sem=send, recv_sem=recv.at[d, s - 1, h, k],
            device_id={"ba": neighbours[d]}, device_id_type=MESH,
        )

    def goes(first, d, s, h, k):
        return s < middle or d == (k if first else h)

    def pass_on(held, send, recv, first, d, s, h, k):
        hop(held, send, recv, d, s, h, k).wait_recv()
        if s < middle and goes(first, d, s + 1, h, k):
            hop(held, send, recv, d, s + 1, h, k).start()

    for k in range(2):
        for r in range(groups):
            @pl.when((k != y) | ((r != 2 * (1 - x)) & (r != a)))
            def _():
                for j in range(pieces):
                    tile_arrival(k, r, j).wait_recv()

        @pl.loop(0, pieces)
        def _(t):
            source = pl.ds(pl.multiple_of(t * piece, 16), piece)
            part = pl.ds(pl.multiple_of(k * half + t * piece, 16), piece)
            gradient = sum(
                jnp.dot(tiles[k, r, source, :], grads[r], preferred_element_type=jnp.float32)
                for r in range(groups)
            )
            updated = 0.95 * momentum[part, :] + gradient
            momentum[part, :] = updated
            scaled = (updated / scale_ref[()]).astype(jnp.bfloat16)
            for h in range(2):
                panel[0, h, part, :] = scaled[:, h * wide : (h + 1) * wide]

    for h, k in by_columns:
        for d in range(2):
            hop(panel, x_send, x_recv, d, 1, h, k).start()

    def span(start, size):
        return pl.ds(pl.multiple_of(start, size), size)

    mine, theirs = c * core_rows + x * share, c * core_rows + (1 - x) * share

    def core_copy(e, h):
        return remote(
            parts.at[e, h, span((1 - c) * core_rows, core_rows)], from_core.at[e, h],
            c_send, c_recv.at[e, h], {"aa": core_mate},
        )

    def chip_copy(e, h):
        return remote(
            parts.at[e, h, span(theirs, share)], from_chip.at[e, h],
            p_send, p_recv.at[e, h], {"aa": chip_mate},
        )

    def share_copy(e, h, step):
        block = gram.at[e, span(h * wide + (theirs if step == 2 else mine), share)]
        return remote(
            block, block, s_send.at[step], s_recv.at[e, h, min(step, 1)],
            {"aa": chip_mate if step == 0 else core_mate},
        )

    def gram_partial(e, h):
        @pl.loop(0, 2)
        def _(q):
            parts[e, h, :, span(q * wide, wide)] = inner_rows(panel[e, h], panel[0, q])

        core_copy(e, h).start()

    def core_sum(e, h):
        core_copy(e, h).wait_recv()
        parts[e, h, span(theirs, share)] += from_core[e, h, span((1 - x) * share, share)]
        chip_copy(e, h).start()
        parts[e, h, span(mine, share)] += from_core[e, h, span(x * share, share)]

    def gram_share(e, h):
        chip_copy(e, h).wait_recv()
        gram[e, span(h * wide + mine, share)] = (
            parts[e, h, span(mine, share)] + from_chip[e, h]
        ).astype(jnp.bfloat16)
        share_copy(e, h, 0).start()
        share_copy(e, h, 1).start()

    def relay(e, h):
        share_copy(e, h, 0).wait_recv()
        share_copy(e, h, 2).start()

    def gram_ready(e, h):
        block = gram.at[e, span(h * wide + (1 - c) * core_rows, core_rows)]
        remote(
            block, block, s_send.at[1], s_recv.at[e, h, 1], {"aa": core_mate}
        ).wait_recv()

    def accumulate(held, e, halves, first, start, count):
        @pl.loop(0, count // half)
        def _(t):
            part = pl.ds(pl.multiple_of(start + t * half, 16), half)
            term = sum(
                jnp.dot(
                    held[e, h, part, :], gram[e, h * wide : (h + 1) * wide, :],
                    preferred_element_type=jnp.float32,
                )
                for h in halves
            )
            if first:
                total[part, :] = term
            else:
                total[part, :] += term

    ring_x = (panel, x_send, x_recv, True)
    last = n - 1
    steps = [[(0, h) for h in range(2)]]
    for s in range(1, middle + 1):
        for h in range(2):
            steps.append([(2 * s - 1, h), (2 * s, h)] if s < middle else [(last, h)])
    final = len(steps) - 1
    for unit in steps[0]:
        gram_partial(*unit)
    for i in range(1, final + 1):
        s, h = (i + 1) // 2, (i + 1) % 2
        for k in range(2):
            for d in range(2):
                if goes(True, d, s, h, k):
                    pass_on(*ring_x, d, s, h, k)
        if i == 1:
            for unit in steps[0]:
                core_sum(*unit)
        for unit in steps[i]:
            gram_partial(*unit)
        if i >= 4:
            for unit in steps[i - 3]:
                relay(*unit)
        if i >= 3:
            for unit in steps[i - 2]:
                gram_share(*unit)
        if i == 3:
            for unit in steps[0]:
                relay(*unit)
        if i == 2:
            for unit in steps[0]:
                gram_share(*unit)
        if i < final:
            for unit in steps[i]:
                core_sum(*unit)
    chores = {
        1: [(core_sum, final)],
        2: [(relay, final - 2)],
        3: [(gram_share, final - 1)],
        6: [(gram_share, final), (relay, final - 1)],
    }
    for e in range(n):
        for do, i in chores.get(e, []):
            for unit in steps[i]:
                do(*unit)
        for h in range(2 if e < last else 1):
            gram_ready(e, h)
        accumulate(panel, e, (0, 1) if e < last else (0,), e == 0, 0, rows)
    relay(last, 1)
    gram_ready(last, 1)

    ring_p = (powers, y_send, y_recv, False)
    for k in range(2):
        part = pl.ds(k * half, half)
        accumulate(panel, last, (1,), False, k * half, half)
        for h in range(2):
            powers[0, h, part, :] = total[part, h * wide : (h + 1) * wide].astype(jnp.bfloat16)
            for d in range(2):
                hop(powers, y_send, y_recv, d, 1, h, k).start()

    accumulate(powers, 0, (0, 1), True, 0, rows)
    for s in range(1, middle):
        for h, k in by_halves:
            for d in range(2):
                pass_on(*ring_p, d, s, h, k)
        for e in (2 * s - 1, 2 * s):
            accumulate(powers, e, (0, 1), False, 0, rows)

    rate = step_ref[()] * factor
    for k in range(2):
        for d in range(2):
            pass_on(*ring_p, d, middle, d, k)
        accumulate(powers, last, (0, 1), False, k * half, half)
        part = pl.ds(k * half, half)
        for h in range(2):
            columns = slice(h * wide, (h + 1) * wide)
            direction = (
                3.4445 * panel[0, h, part, :].astype(jnp.float32)
                - 4.775 * powers[0, h, part, :].astype(jnp.float32)
                + 2.0315 * total[part, columns]
            )
            weight[part, columns] = weight[part, columns] - rate * direction

    def sent(block, send):
        remote(block, block, send, x_recv.at[0, 0, 0, 0], {"aa": core_mate}).wait_send()

    sent(panel.at[pl.ds(1, n - 1)], x_send)
    sent(powers.at[pl.ds(1, n - 1)], y_send)
    sent(from_core, c_send)
    sent(from_chip, p_send)
    for step in range(3):
        sent(gram.at[pl.ds(0, n // groups)], s_send.at[step])
    for kind in range(3):
        grad_copy(kind).wait_send()
    sent(line.at[pl.ds(0, layers - 1)], t_send.at[0])
    sent(line.at[pl.ds(0, 2)], t_send.at[1])
    sent(line.at[0], t_send.at[2])

    @pl.when(c == 1)
    def _():
        sent(line.at[pl.ds(0, 2)], t_send.at[3])
        sent(line.at[pl.ds(0, 2)], t_send.at[4])

    for layer in range(layers):
        for side in range(2):
            from_here = layer <= z if side == 0 else layer >= z

            @pl.when(from_here & can_go[side])
            def _():
                sent(line.at[layer], z_send.at[side, layer])


def fused_step(activations, out_grad, momentum, weight, norm_scale, step_size, n, groups):
    tokens, features = activations.shape
    rows, width = momentum.shape
    wide, middle = width // 2, n // 2
    pieces = 3 if features % 48 == 0 else 1
    dma = pltpu.SemaphoreType.DMA
    vmem = pl.BlockSpec(memory_space=pltpu.VMEM)
    hbm = pl.BlockSpec(memory_space=pltpu.HBM)
    smem = pl.BlockSpec(memory_space=pltpu.SMEM)
    ring = dma((2, middle, 2, 2))
    units = dma((n, 2))
    return pl.pallas_call(
        functools.partial(step_kernel, n, groups, 0.2 * math.sqrt(max(ROWS, COLS))),
        out_shape=(
            jax.ShapeDtypeStruct((rows, width), jnp.float32),
            jax.ShapeDtypeStruct((rows, width), jnp.float32),
        ),
        in_specs=[hbm, hbm, hbm, hbm, smem, smem],
        out_specs=(vmem, vmem),
        scratch_shapes=[
            pltpu.VMEM((n // 2, features, tokens), jnp.bfloat16),
            pltpu.VMEM((2, features, tokens), jnp.bfloat16),
            pltpu.VMEM((2, groups, features, tokens), jnp.bfloat16),
            pltpu.VMEM((groups, tokens, width), jnp.bfloat16),
            pltpu.VMEM((n, 2, rows, wide), jnp.bfloat16),
            pltpu.VMEM((n, 2, rows, wide), jnp.bfloat16),
            pltpu.VMEM((n, width, width), jnp.bfloat16),
            pltpu.VMEM((n, 2, wide, width), jnp.float32),
            pltpu.VMEM((n, 2, wide // 2, width), jnp.float32),
            pltpu.VMEM((n, 2, wide // groups, width), jnp.float32),
            pltpu.VMEM((rows, width), jnp.float32),
            dma((2, n // 2)), dma((n // 2, pieces)),
            dma((5,)), dma((2, groups, pieces)), dma((2, pieces)),
            dma((3,)), dma((3,)),
            dma, ring, dma, ring,
            dma, units, dma, units,
            dma((3,)), dma((n, 2, 2)),
            dma((4,)),
        ],
        compiler_params=pltpu.CompilerParams(
            collective_id=0, has_side_effects=True, vmem_limit_bytes=48 * 1024 * 1024
        ),
        name="step",
    )(
        pltpu.with_memory_space_constraint(activations.T, pltpu.HBM),
        pltpu.with_memory_space_constraint(out_grad, pltpu.HBM), momentum, weight, norm_scale, step_size)


def plain_gradient(activations, out_grad):
    features = lax.all_to_all(
        lax.all_gather(activations, "ba", axis=1, tiled=True),
        "aa", split_axis=1, concat_axis=0, tiled=True,
    )
    return inner_rows(features, lax.all_gather(out_grad, "aa", axis=0, tiled=True))


def plain_direction(scaled):
    row_panel = lax.all_gather(scaled, "ba", axis=1, tiled=True)
    gram_part = inner_rows(row_panel, scaled)
    width = gram_part.shape[0]
    groups = lax.axis_size("aa")
    padding = (groups - width % groups) % groups
    padded = jnp.pad(gram_part, ((0, padding), (0, 0)))
    share = lax.psum_scatter(padded, "aa", scatter_dimension=0, tiled=True).astype(jnp.bfloat16)
    gram_cols = lax.all_gather(share, "aa", axis=0, tiled=True)[:width]
    first_power = jnp.dot(row_panel, gram_cols, preferred_element_type=jnp.float32).astype(
        jnp.bfloat16
    )
    second_power = jnp.dot(
        lax.all_gather(first_power, "ba", axis=1, tiled=True),
        gram_cols,
        preferred_element_type=jnp.float32,
    )
    return (
        3.4445 * scaled.astype(jnp.float32)
        - 4.775 * first_power.astype(jnp.float32)
        + 2.0315 * second_power
    )


def per_device(activations, out_grad, momentum, weight, norm_scale, step_size):
    n, groups = lax.axis_size("ba"), lax.axis_size("aa")
    rows, width = momentum.shape
    tokens, features = activations.shape
    fits = (
        groups == 4 and n == 2 * groups and rows == 2 * features
        and features % 16 == 0 and tokens % 128 == 0 and width % 256 == 0
        and width % (32 * groups) == 0
        and 4 * n * rows * width + 9 * n * width * width + 17 * rows * width < 56 * 2**20
    )
    if fits:
        return fused_step(
            activations, out_grad, momentum, weight, norm_scale, step_size, n, groups
        )
    new_momentum = 0.95 * momentum + plain_gradient(activations, out_grad)
    scaled = (new_momentum / norm_scale).astype(jnp.bfloat16)
    factor = 0.2 * math.sqrt(max(ROWS, COLS))
    new_weight = weight - step_size * factor * plain_direction(scaled)
    return (new_weight, new_momentum)


def solution(mesh):
    placed = (P("aa", "ba"), P("aa", "ba"), P("aa", "ba"), P("aa", "ba"), P(), P())
    return jax.shard_map(
        per_device,
        mesh=mesh,
        in_specs=placed,
        out_specs=(P("aa", "ba"), P("aa", "ba")),
        check_vma=False,
    )
```

```python
import functools
import math

import jax
import jax.numpy as jnp
from jax import lax
from jax.experimental import pallas as pl
from jax.experimental.pallas import tpu as pltpu
from jax.sharding import PartitionSpec as P

ROWS = 4224
COLS = 4096
MESH = pl.DeviceIdType.MESH


def inner_rows(left, right):
    return lax.dot_general(
        left, right, (((0,), (0,)), ((), ())), preferred_element_type=jnp.float32
    )


def step_kernel(
    n, groups, factor,
    act_hbm, grad_hbm, momentum_hbm, weight_hbm, scale_ref, step_ref,
    weight, momentum,
    line, stage, tiles, grads, panel, powers, gram, parts, from_core, from_chip, total,
    z_send, z_recv, t_send, t_recv, b_recv, g_send, g_recv,
    x_send, x_recv, y_send, y_recv, c_send, c_recv, p_send, p_recv, s_send, s_recv,
    load_sem,
):
    half = line.shape[1]
    rows, width = momentum.shape
    wide, middle, layers = width // 2, n // 2, n // 2
    core_rows, share = wide // 2, wide // groups
    pieces = 3 if half % 48 == 0 else 1
    a, b = lax.axis_index("aa"), lax.axis_index("ba")
    x, c, z, y = a // 2, a % 2, b // 2, b % 2
    core_mate = 2 * x + 1 - c
    chip_mate = 2 * (1 - x) + c
    y_mate = 2 * z + 1 - y

    loads = [
        pltpu.make_async_copy(act_hbm, line.at[z], load_sem.at[0]),
        pltpu.make_async_copy(grad_hbm, grads.at[a], load_sem.at[1]),
        pltpu.make_async_copy(momentum_hbm, momentum, load_sem.at[2]),
        pltpu.make_async_copy(weight_hbm, weight, load_sem.at[3]),
    ]
    for load in loads:
        load.start()

    place = z + y * (n - 1 - 2 * z)

    def at(position):
        position = (position + n) % n
        column = position // middle
        return 2 * (position + column * (n - 1 - 2 * position)) + column

    neighbours = (at(place + 1), at(place - 1))

    barrier = pltpu.get_barrier_semaphore()
    for r in range(1, groups):
        pl.semaphore_signal(barrier, 1, device_id={"aa": (a + r) % groups}, device_id_type=MESH)
    for r in range(groups):
        pl.semaphore_signal(
            barrier, 1, device_id={"aa": (a + r) % groups, "ba": y_mate}, device_id_type=MESH
        )

    @pl.when(z > 0)
    def _():
        pl.semaphore_signal(barrier, 1, device_id={"ba": b - 2}, device_id_type=MESH)

    @pl.when(z < layers - 1)
    def _():
        pl.semaphore_signal(barrier, 1, device_id={"ba": b + 2}, device_id_type=MESH)

    sides = (z + layers - 1) // layers + (2 * layers - 2 - z) // layers
    pl.semaphore_wait(barrier, 2 * groups - 1 + sides)

    piece = half // pieces

    def cut(j):
        return pl.ds(j * piece, piece)

    def remote(source, target, send, recv, where):
        return pltpu.make_async_remote_copy(
            src_ref=source, dst_ref=target, send_sem=send, recv_sem=recv,
            device_id=where, device_id_type=MESH,
        )

    def z_hop(layer, side, j):
        block = line.at[layer, cut(j)]
        return remote(
            block, block, z_send.at[side, layer], z_recv.at[layer, j], {"ba": b + 2 - 4 * side}
        )

    def near_copy(layer, j):
        return remote(
            line.at[layer, cut(j)], tiles.at[y, a, cut(j)], t_send.at[0], t_recv.at[y, a, j],
            {"aa": layer},
        )

    def far_copy(layer, j):
        return remote(
            line.at[layer, cut(j)], tiles.at[y, a, cut(j)], t_send.at[1], t_recv.at[y, a, j],
            {"aa": layer, "ba": y_mate},
        )

    def relay_copy(j):
        block = tiles.at[y, 2 * (1 - x), cut(j)]
        return remote(block, block, t_send.at[2], t_recv.at[y, 2 * (1 - x), j], {"ba": y_mate})

    def side_copy(layer, j):
        return remote(
            line.at[layer, cut(j)], stage.at[layer % 2, cut(j)], t_send.at[3],
            b_recv.at[layer % 2, j], {"ba": y_mate},
        )

    def cross_copy(slot, j):
        return remote(
            stage.at[slot, cut(j)], tiles.at[1 - y, a, cut(j)], t_send.at[4],
            t_recv.at[1 - y, a, j], {"aa": 2 * (1 - x) + slot},
        )

    def tile_arrival(k, r, j):
        block = tiles.at[k, r, cut(j)]
        return remote(block, block, t_send.at[0], t_recv.at[k, r, j], {"aa": core_mate})

    def deliver(layer, j):
        pl.when(layer // 2 == x)(far_copy(layer, j).start)
        pl.when((layer // 2 != x) & (c == 1))(side_copy(layer, j).start)
        pl.when(layer != a)(near_copy(layer, j).start)

        @pl.when(layer == a)
        def _():
            tiles[y, a, cut(j)] = line[layer, cut(j)]

    def grad_copy(kind):
        slot = chip_mate if kind == 2 else a
        return remote(
            grads.at[slot], grads.at[slot], g_send.at[kind], g_recv.at[kind],
            {"aa": chip_mate if kind == 0 else core_mate},
        )

    loads[0].wait()
    loads[1].wait()
    can_go = (z < layers - 1, z > 0)
    for j in range(pieces):
        for side in range(2):
            pl.when(can_go[side])(z_hop(z, side, j).start)
        deliver(z, j)
        if j == 0:
            grad_copy(0).start()
            grad_copy(1).start()
    for distance in range(1, layers + 1):
        if distance < layers:
            for j in range(pieces):
                for side in range(2):
                    layer = z - distance if side == 0 else z + distance

                    @pl.when((layer >= 0) & (layer < layers))
                    def _():
                        z_hop(layer, side, j).wait_recv()
                        pl.when(can_go[side])(z_hop(layer, side, j).start)
                        deliver(layer, j)

        for side in range(2):
            layer = z - distance + 1 if side == 0 else z + distance - 1
            there = (layer >= 0) & (layer < layers) & ((side == 0) | (distance > 1))

            @pl.when(there & (layer // 2 != x) & (c == 1))
            def _():
                for j in range(pieces):
                    side_copy(layer, j).wait_recv()
                    cross_copy(layer % 2, j).start()

        @pl.when((z - a == distance - 1) | (a - z == distance - 1))
        def _():
            for j in range(pieces):
                tile_arrival(y, 2 * (1 - x), j).wait_recv()
                relay_copy(j).start()

        if distance == 1:
            grad_copy(0).wait_recv()
            grad_copy(2).start()
    grad_copy(1).wait_recv()
    grad_copy(2).wait_recv()
    loads[2].wait()
    loads[3].wait()

    by_columns = [(h, k) for h in range(2) for k in range(2)]
    by_halves = [(h, k) for k in range(2) for h in range(2)]

    def row_half(position, k):
        position = (position + n) % n
        return pl.ds(pl.multiple_of((position // middle + k) % 2 * half, 16), half)

    def hop(held, send, recv, first, d, s, h, k, arrival=False):
        target = n - 1 if s == middle else 2 * s - 1 + d
        origin = 0 if s == 1 else 2 * s - 3 + d
        steps_back = s if arrival else s - 1
        part = row_half(place - steps_back + 2 * d * steps_back, k) if first else pl.ds(k * half, half)
        return remote(
            held.at[origin, h, part], held.at[target, h, part], send, recv.at[d, s - 1, h, k],
            {"ba": neighbours[d]},
        )

    def goes(first, d, s, h, k):
        return s < middle or d == (k if first else h)

    def pass_on(held, send, recv, first, d, s, h, k):
        hop(held, send, recv, first, d, s, h, k, arrival=True).wait_recv()
        if s < middle and goes(first, d, s + 1, h, k):
            hop(held, send, recv, first, d, s + 1, h, k).start()

    ring_x = (panel, x_send, x_recv, True)
    for k in range(2):
        owner = y if k == 0 else 1 - y
        for r in range(groups):
            @pl.when((r != 2 * (1 - x)) & (r != a) if k == 0 else r >= 0)
            def _():
                for j in range(pieces):
                    tile_arrival(owner, r, j).wait_recv()

        @pl.loop(0, pieces)
        def _(t):
            source = pl.ds(pl.multiple_of(t * piece, 16), piece)
            part = pl.ds(pl.multiple_of(owner * half + t * piece, 16), piece)
            gradient = sum(
                jnp.dot(tiles[owner, r, source, :], grads[r], preferred_element_type=jnp.float32)
                for r in range(groups)
            )
            updated = 0.95 * momentum[part, :] + gradient
            momentum[part, :] = updated
            scaled = (updated / scale_ref[()]).astype(jnp.bfloat16)
            for h in range(2):
                panel[0, h, part, :] = scaled[:, h * wide : (h + 1) * wide]

        if k == 0:
            for d in range(2):
                hop(*ring_x, d, 1, 0, 0).start()

    for h, k in by_columns[1:]:
        for d in range(2):
            hop(*ring_x, d, 1, h, k).start()

    def span(start, size):
        return pl.ds(pl.multiple_of(start, size), size)

    mine, theirs = c * core_rows + x * share, c * core_rows + (1 - x) * share

    def core_copy(e, h):
        return remote(
            parts.at[e, h, span((1 - c) * core_rows, core_rows)], from_core.at[e, h],
            c_send, c_recv.at[e, h], {"aa": core_mate},
        )

    def chip_copy(e, h):
        return remote(
            parts.at[e, h, span(theirs, share)], from_chip.at[e, h],
            p_send, p_recv.at[e, h], {"aa": chip_mate},
        )

    def share_copy(e, h, step):
        block = gram.at[e, span(h * wide + (theirs if step == 2 else mine), share)]
        return remote(
            block, block, s_send.at[step], s_recv.at[e, h, min(step, 1)],
            {"aa": chip_mate if step == 0 else core_mate},
        )

    def gram_partial(e, h):
        @pl.loop(0, 2)
        def _(q):
            parts[e, h, :, span(q * wide, wide)] = inner_rows(panel[e, h], panel[0, q])

        core_copy(e, h).start()

    def core_sum(e, h):
        core_copy(e, h).wait_recv()
        parts[e, h, span(theirs, share)] += from_core[e, h, span((1 - x) * share, share)]
        chip_copy(e, h).start()
        parts[e, h, span(mine, share)] += from_core[e, h, span(x * share, share)]

    def gram_share(e, h):
        chip_copy(e, h).wait_recv()
        gram[e, span(h * wide + mine, share)] = (
            parts[e, h, span(mine, share)] + from_chip[e, h]
        ).astype(jnp.bfloat16)
        share_copy(e, h, 0).start()
        share_copy(e, h, 1).start()

    def relay(e, h):
        share_copy(e, h, 0).wait_recv()
        share_copy(e, h, 2).start()

    def gram_ready(e, h):
        block = gram.at[e, span(h * wide + (1 - c) * core_rows, core_rows)]
        remote(
            block, block, s_send.at[1], s_recv.at[e, h, 1], {"aa": core_mate}
        ).wait_recv()

    def accumulate(held, e, halves, first, start, count):
        @pl.loop(0, count // half)
        def _(t):
            part = pl.ds(pl.multiple_of(start + t * half, 16), half)
            term = sum(
                jnp.dot(
                    held[e, h, part, :], gram[e, h * wide : (h + 1) * wide, :],
                    preferred_element_type=jnp.float32,
                )
                for h in halves
            )
            if first:
                total[part, :] = term
            else:
                total[part, :] += term

    last = n - 1
    steps = [[(0, h) for h in range(2)]]
    for s in range(1, middle + 1):
        for h in range(2):
            steps.append([(2 * s - 1, h), (2 * s, h)] if s < middle else [(last, h)])
    final = len(steps) - 1

    def each(do, i):
        for unit in steps[i]:
            do(*unit)

    each(gram_partial, 0)
    for i in range(1, final + 1):
        s, h = (i + 1) // 2, (i + 1) % 2
        for k in range(2):
            for d in range(2):
                if goes(True, d, s, h, k):
                    pass_on(*ring_x, d, s, h, k)
            if k == 0 and 1 < i < final - 1:
                each(gram_share, i - 1)
        if i == 1:
            each(core_sum, 0)
        each(gram_partial, i)
        if i == 2:
            each(gram_share, 0)
        each(core_sum, i)
        if i == 3:
            each(relay, 0)
        if 1 < i < final - 1:
            each(relay, i - 1)
        if i == final - 1:
            each(gram_share, i - 1)
    each(relay, final - 2)
    each(gram_share, final - 1)
    for e in range(n):
        if e == 4:
            each(gram_share, final)
        if e == 5:
            each(relay, final - 1)
        for h in range(2 if e < last else 1):
            gram_ready(e, h)
        accumulate(panel, e, (0, 1) if e < last else (0,), e == 0, 0, rows)
    relay(last, 1)
    gram_ready(last, 1)

    ring_p = (powers, y_send, y_recv, False)
    for k in range(2):
        part = pl.ds(k * half, half)
        accumulate(panel, last, (1,), False, k * half, half)
        for h in range(2):
            powers[0, h, part, :] = total[part, h * wide : (h + 1) * wide].astype(jnp.bfloat16)
            for d in range(2):
                hop(*ring_p, d, 1, h, k).start()

    accumulate(powers, 0, (0, 1), True, 0, rows)
    for s in range(1, middle):
        for h, k in by_halves:
            for d in range(2):
                pass_on(*ring_p, d, s, h, k)
        for e in (2 * s - 1, 2 * s):
            accumulate(powers, e, (0, 1), False, 0, rows)

    rate = step_ref[()] * factor
    for k in range(2):
        for d in range(2):
            pass_on(*ring_p, d, middle, d, k)
        accumulate(powers, last, (0, 1), False, k * half, half)
        part = pl.ds(k * half, half)
        for h in range(2):
            columns = slice(h * wide, (h + 1) * wide)
            direction = (
                3.4445 * panel[0, h, part, :].astype(jnp.float32)
                - 4.775 * powers[0, h, part, :].astype(jnp.float32)
                + 2.0315 * total[part, columns]
            )
            weight[part, columns] = weight[part, columns] - rate * direction

    def sent(block, send):
        remote(block, block, send, x_recv.at[0, 0, 0, 0], {"aa": core_mate}).wait_send()

    sent(panel.at[pl.ds(1, n - 1)], x_send)
    sent(powers.at[pl.ds(1, n - 1)], y_send)
    sent(from_core, c_send)
    sent(from_chip, p_send)
    for step in range(3):
        sent(gram.at[pl.ds(0, n // groups)], s_send.at[step])
    for kind in range(3):
        grad_copy(kind).wait_send()
    sent(line.at[pl.ds(0, layers - 1)], t_send.at[0])
    sent(line.at[pl.ds(0, 2)], t_send.at[1])
    sent(line.at[0], t_send.at[2])

    @pl.when(c == 1)
    def _():
        sent(line.at[pl.ds(0, 2)], t_send.at[3])
        sent(line.at[pl.ds(0, 2)], t_send.at[4])

    for layer in range(layers):
        for side in range(2):
            from_here = layer <= z if side == 0 else layer >= z

            @pl.when(from_here & can_go[side])
            def _():
                sent(line.at[layer], z_send.at[side, layer])


def fused_step(activations, out_grad, momentum, weight, norm_scale, step_size, n, groups):
    tokens, features = activations.shape
    rows, width = momentum.shape
    wide, middle = width // 2, n // 2
    pieces = 3 if features % 48 == 0 else 1
    dma = pltpu.SemaphoreType.DMA
    vmem = pl.BlockSpec(memory_space=pltpu.VMEM)
    hbm = pl.BlockSpec(memory_space=pltpu.HBM)
    smem = pl.BlockSpec(memory_space=pltpu.SMEM)
    ring = dma((2, middle, 2, 2))
    units = dma((n, 2))
    return pl.pallas_call(
        functools.partial(step_kernel, n, groups, 0.2 * math.sqrt(max(ROWS, COLS))),
        out_shape=(
            jax.ShapeDtypeStruct((rows, width), jnp.float32),
            jax.ShapeDtypeStruct((rows, width), jnp.float32),
        ),
        in_specs=[hbm, hbm, hbm, hbm, smem, smem],
        out_specs=(vmem, vmem),
        scratch_shapes=[
            pltpu.VMEM((n // 2, features, tokens), jnp.bfloat16),
            pltpu.VMEM((2, features, tokens), jnp.bfloat16),
            pltpu.VMEM((2, groups, features, tokens), jnp.bfloat16),
            pltpu.VMEM((groups, tokens, width), jnp.bfloat16),
            pltpu.VMEM((n, 2, rows, wide), jnp.bfloat16),
            pltpu.VMEM((n, 2, rows, wide), jnp.bfloat16),
            pltpu.VMEM((n, width, width), jnp.bfloat16),
            pltpu.VMEM((n, 2, wide, width), jnp.float32),
            pltpu.VMEM((n, 2, wide // 2, width), jnp.float32),
            pltpu.VMEM((n, 2, wide // groups, width), jnp.float32),
            pltpu.VMEM((rows, width), jnp.float32),
            dma((2, n // 2)), dma((n // 2, pieces)),
            dma((5,)), dma((2, groups, pieces)), dma((2, pieces)),
            dma((3,)), dma((3,)),
            dma, ring, dma, ring,
            dma, units, dma, units,
            dma((3,)), dma((n, 2, 2)),
            dma((4,)),
        ],
        compiler_params=pltpu.CompilerParams(
            collective_id=0, has_side_effects=True, vmem_limit_bytes=48 * 1024 * 1024
        ),
        name="step",
    )(
        pltpu.with_memory_space_constraint(activations.T, pltpu.HBM),
        pltpu.with_memory_space_constraint(out_grad, pltpu.HBM), momentum, weight, norm_scale, step_size)


def plain_gradient(activations, out_grad):
    features = lax.all_to_all(
        lax.all_gather(activations, "ba", axis=1, tiled=True),
        "aa", split_axis=1, concat_axis=0, tiled=True,
    )
    return inner_rows(features, lax.all_gather(out_grad, "aa", axis=0, tiled=True))


def plain_direction(scaled):
    row_panel = lax.all_gather(scaled, "ba", axis=1, tiled=True)
    gram_part = inner_rows(row_panel, scaled)
    width = gram_part.shape[0]
    groups = lax.axis_size("aa")
    padding = (groups - width % groups) % groups
    padded = jnp.pad(gram_part, ((0, padding), (0, 0)))
    share = lax.psum_scatter(padded, "aa", scatter_dimension=0, tiled=True).astype(jnp.bfloat16)
    gram_cols = lax.all_gather(share, "aa", axis=0, tiled=True)[:width]
    first_power = jnp.dot(row_panel, gram_cols, preferred_element_type=jnp.float32).astype(
        jnp.bfloat16
    )
    second_power = jnp.dot(
        lax.all_gather(first_power, "ba", axis=1, tiled=True),
        gram_cols,
        preferred_element_type=jnp.float32,
    )
    return (
        3.4445 * scaled.astype(jnp.float32)
        - 4.775 * first_power.astype(jnp.float32)
        + 2.0315 * second_power
    )


def per_device(activations, out_grad, momentum, weight, norm_scale, step_size):
    n, groups = lax.axis_size("ba"), lax.axis_size("aa")
    rows, width = momentum.shape
    tokens, features = activations.shape
    fits = (
        groups == 4 and n == 2 * groups and rows == 2 * features
        and features % 16 == 0 and tokens % 128 == 0 and width % 256 == 0
        and width % (32 * groups) == 0
        and 4 * n * rows * width + 9 * n * width * width + 17 * rows * width < 56 * 2**20
    )
    if fits:
        return fused_step(
            activations, out_grad, momentum, weight, norm_scale, step_size, n, groups
        )
    new_momentum = 0.95 * momentum + plain_gradient(activations, out_grad)
    scaled = (new_momentum / norm_scale).astype(jnp.bfloat16)
    factor = 0.2 * math.sqrt(max(ROWS, COLS))
    new_weight = weight - step_size * factor * plain_direction(scaled)
    return (new_weight, new_momentum)


def solution(mesh):
    placed = (P("aa", "ba"), P("aa", "ba"), P("aa", "ba"), P("aa", "ba"), P(), P())
    return jax.shard_map(
        per_device,
        mesh=mesh,
        in_specs=placed,
        out_specs=(P("aa", "ba"), P("aa", "ba")),
        check_vma=False,
    )
```

```python
import functools
import math

import jax
import jax.numpy as jnp
from jax import lax
from jax.experimental import pallas as pl
from jax.experimental.pallas import tpu as pltpu
from jax.sharding import PartitionSpec as P

ROWS = 4224
COLS = 4096
MESH = pl.DeviceIdType.MESH


def inner_rows(left, right):
    return lax.dot_general(
        left, right, (((0,), (0,)), ((), ())), preferred_element_type=jnp.float32
    )


def step_kernel(
    n, groups, factor,
    act_hbm, grad_hbm, momentum_hbm, weight_hbm, scale_ref, step_ref,
    weight, momentum,
    line, stage, tiles, grads, panel, powers, gram, parts, from_core, from_chip, total,
    z_send, z_recv, t_send, t_recv, b_recv, g_send, g_recv,
    x_send, x_recv, y_send, y_recv, c_send, c_recv, p_send, p_recv, s_send, s_recv,
    load_sem,
):
    half = line.shape[1]
    rows, width = momentum.shape
    wide, middle, layers = width // 2, n // 2, n // 2
    narrow = wide // 2
    pieces = 3 if half % 48 == 0 else 1
    a, b = lax.axis_index("aa"), lax.axis_index("ba")
    x, c, z, y = a // 2, a % 2, b // 2, b % 2
    core_mate = 2 * x + 1 - c
    chip_mate = 2 * (1 - x) + c
    y_mate = 2 * z + 1 - y

    loads = [
        pltpu.make_async_copy(act_hbm, line.at[z], load_sem.at[0]),
        pltpu.make_async_copy(grad_hbm, grads.at[a], load_sem.at[1]),
        pltpu.make_async_copy(momentum_hbm, momentum, load_sem.at[2]),
        pltpu.make_async_copy(weight_hbm, weight, load_sem.at[3]),
    ]
    for load in loads:
        load.start()

    place = z + y * (n - 1 - 2 * z)

    def at(position):
        position = (position + n) % n
        column = position // middle
        return 2 * (position + column * (n - 1 - 2 * position)) + column

    neighbours = (at(place + 1), at(place - 1))

    barrier = pltpu.get_barrier_semaphore()
    for r in range(1, groups):
        pl.semaphore_signal(barrier, 1, device_id={"aa": (a + r) % groups}, device_id_type=MESH)
    for r in range(groups):
        pl.semaphore_signal(
            barrier, 1, device_id={"aa": (a + r) % groups, "ba": y_mate}, device_id_type=MESH
        )

    @pl.when(z > 0)
    def _():
        pl.semaphore_signal(barrier, 1, device_id={"ba": b - 2}, device_id_type=MESH)

    @pl.when(z < layers - 1)
    def _():
        pl.semaphore_signal(barrier, 1, device_id={"ba": b + 2}, device_id_type=MESH)

    sides = (z + layers - 1) // layers + (2 * layers - 2 - z) // layers
    pl.semaphore_wait(barrier, 2 * groups - 1 + sides)

    piece = half // pieces

    def cut(j):
        return pl.ds(j * piece, piece)

    def remote(source, target, send, recv, where):
        return pltpu.make_async_remote_copy(
            src_ref=source, dst_ref=target, send_sem=send, recv_sem=recv,
            device_id=where, device_id_type=MESH,
        )

    def z_hop(layer, side, j):
        block = line.at[layer, cut(j)]
        return remote(
            block, block, z_send.at[side, layer], z_recv.at[layer, j], {"ba": b + 2 - 4 * side}
        )

    def near_copy(layer, j):
        return remote(
            line.at[layer, cut(j)], tiles.at[y, a, cut(j)], t_send.at[0], t_recv.at[y, a, j],
            {"aa": layer},
        )

    def far_copy(layer, j):
        return remote(
            line.at[layer, cut(j)], tiles.at[y, a, cut(j)], t_send.at[1], t_recv.at[y, a, j],
            {"aa": layer, "ba": y_mate},
        )

    def relay_copy(j):
        block = tiles.at[y, 2 * (1 - x), cut(j)]
        return remote(block, block, t_send.at[2], t_recv.at[y, 2 * (1 - x), j], {"ba": y_mate})

    def side_copy(layer, j):
        return remote(
            line.at[layer, cut(j)], stage.at[layer % 2, cut(j)], t_send.at[3],
            b_recv.at[layer % 2, j], {"ba": y_mate},
        )

    def cross_copy(slot, j):
        return remote(
            stage.at[slot, cut(j)], tiles.at[1 - y, a, cut(j)], t_send.at[4],
            t_recv.at[1 - y, a, j], {"aa": 2 * (1 - x) + slot},
        )

    def tile_arrival(k, r, j):
        block = tiles.at[k, r, cut(j)]
        return remote(block, block, t_send.at[0], t_recv.at[k, r, j], {"aa": core_mate})

    def deliver(layer, j):
        pl.when(layer // 2 == x)(far_copy(layer, j).start)
        pl.when((layer // 2 != x) & (c == 1))(side_copy(layer, j).start)
        pl.when(layer != a)(near_copy(layer, j).start)

        @pl.when(layer == a)
        def _():
            tiles[y, a, cut(j)] = line[layer, cut(j)]

    def grad_copy(kind):
        slot = chip_mate if kind == 2 else a
        return remote(
            grads.at[slot], grads.at[slot], g_send.at[kind], g_recv.at[kind],
            {"aa": chip_mate if kind == 0 else core_mate},
        )

    loads[0].wait()
    loads[1].wait()
    can_go = (z < layers - 1, z > 0)
    for j in range(pieces):
        for side in range(2):
            pl.when(can_go[side])(z_hop(z, side, j).start)
        deliver(z, j)
        if j == 0:
            grad_copy(0).start()
            grad_copy(1).start()
    for distance in range(1, layers + 1):
        if distance < layers:
            for j in range(pieces):
                for side in range(2):
                    layer = z - distance if side == 0 else z + distance

                    @pl.when((layer >= 0) & (layer < layers))
                    def _():
                        z_hop(layer, side, j).wait_recv()
                        pl.when(can_go[side])(z_hop(layer, side, j).start)
                        deliver(layer, j)

        for side in range(2):
            layer = z - distance + 1 if side == 0 else z + distance - 1
            there = (layer >= 0) & (layer < layers) & ((side == 0) | (distance > 1))

            @pl.when(there & (layer // 2 != x) & (c == 1))
            def _():
                for j in range(pieces):
                    side_copy(layer, j).wait_recv()
                    cross_copy(layer % 2, j).start()

        @pl.when((z - a == distance - 1) | (a - z == distance - 1))
        def _():
            for j in range(pieces):
                tile_arrival(y, 2 * (1 - x), j).wait_recv()
                relay_copy(j).start()

        if distance == 1:
            grad_copy(0).wait_recv()
            grad_copy(2).start()
    grad_copy(1).wait_recv()
    grad_copy(2).wait_recv()
    loads[2].wait()
    loads[3].wait()

    def row_half(position, k):
        position = (position + n) % n
        return pl.ds(pl.multiple_of((position // middle + k) % 2 * half, 16), half)

    def hop_x(d, s, p, arrival=False):
        target = n - 1 if s == middle else 2 * s - 1 + d
        origin = 0 if s == 1 else 2 * s - 3 + d
        if p < 2:
            back = s if arrival else s - 1
            cut_out = (0, row_half(place - back + 2 * d * back, p))
        else:
            cut_out = (
                1, pl.ds(d * half, half) if s == middle else pl.ds(0, rows),
                pl.ds((p - 2) * narrow, narrow),
            )
        return remote(
            panel.at[(origin, *cut_out)], panel.at[(target, *cut_out)],
            x_send, x_recv.at[d, s - 1, p], {"ba": neighbours[d]},
        )

    def goes_x(d, s, p):
        return s < middle or p > 1 or d == p

    def pass_x(s, p):
        for d in range(2):
            if goes_x(d, s, p):
                hop_x(d, s, p, arrival=True).wait_recv()
                if s < middle and goes_x(d, s + 1, p):
                    hop_x(d, s + 1, p).start()

    def hop_p(d, s, h, k):
        target = n - 1 if s == middle else 2 * s - 1 + d
        origin = 0 if s == 1 else 2 * s - 3 + d
        part = pl.ds(k * half, half)
        return remote(
            powers.at[origin, h, part], powers.at[target, h, part],
            y_send, y_recv.at[d, s - 1, h, k], {"ba": neighbours[d]},
        )

    def pass_p(d, s, h, k):
        hop_p(d, s, h, k).wait_recv()
        if s + 1 < middle or (s + 1 == middle and d == h):
            hop_p(d, s + 1, h, k).start()

    for k in range(2):
        owner = y if k == 0 else 1 - y
        for r in range(groups):
            @pl.when((r != 2 * (1 - x)) & (r != a) if k == 0 else r >= 0)
            def _():
                for j in range(pieces):
                    tile_arrival(owner, r, j).wait_recv()

        @pl.loop(0, pieces)
        def _(t):
            source = pl.ds(pl.multiple_of(t * piece, 16), piece)
            part = pl.ds(pl.multiple_of(owner * half + t * piece, 16), piece)
            gradient = sum(
                jnp.dot(tiles[owner, r, source, :], grads[r], preferred_element_type=jnp.float32)
                for r in range(groups)
            )
            updated = 0.95 * momentum[part, :] + gradient
            momentum[part, :] = updated
            scaled = (updated / scale_ref[()]).astype(jnp.bfloat16)
            for h in range(2):
                panel[0, h, part, :] = scaled[:, h * wide : (h + 1) * wide]

        if k == 0:
            for d in range(2):
                hop_x(d, 1, 0).start()

    for p in range(1, 4):
        for d in range(2):
            hop_x(d, 1, p).start()

    def span(start, size):
        return pl.ds(pl.multiple_of(start, 16), size)

    sizes, starts = (wide, narrow, narrow), (0, wide, wide + narrow)

    def rows_of(u, core, chip):
        return starts[u] + core * (sizes[u] // 2) + chip * (sizes[u] // groups)

    def core_half(u, core):
        return span(rows_of(u, core, 0), sizes[u] // 2)

    def part_of(u, core, chip):
        return span(rows_of(u, core, chip), sizes[u] // groups)

    def chip_part(u, chip):
        return span(starts[u] // 2 + chip * (sizes[u] // groups), sizes[u] // groups)

    def core_copy(e, u):
        return remote(
            parts.at[e, core_half(u, 1 - c)], from_core.at[e, pl.ds(starts[u] // 2, sizes[u] // 2)],
            c_send, c_recv.at[e, u], {"aa": core_mate},
        )

    def chip_copy(e, u):
        return remote(
            parts.at[e, part_of(u, c, 1 - x)],
            from_chip.at[e, pl.ds(starts[u] // groups, sizes[u] // groups)],
            p_send, p_recv.at[e, u], {"aa": chip_mate},
        )

    def share_copy(e, u, step):
        block = gram.at[e, part_of(u, c, 1 - x if step == 2 else x)]
        return remote(
            block, block, s_send.at[step], s_recv.at[e, u, min(step, 1)],
            {"aa": chip_mate if step == 0 else core_mate},
        )

    def gram_partial(e, u):
        h = min(u, 1)
        first = starts[u] - h * wide

        @pl.loop(0, 2)
        def _(q):
            parts[e, pl.ds(starts[u], sizes[u]), pl.ds(pl.multiple_of(q * wide, wide), wide)] = (
                inner_rows(panel[e, h, :, first : first + sizes[u]], panel[0, q])
            )

        core_copy(e, u).start()

    def core_sum(e, u):
        core_copy(e, u).wait_recv()
        parts[e, part_of(u, c, 1 - x)] += from_core[e, chip_part(u, 1 - x)]
        chip_copy(e, u).start()
        parts[e, part_of(u, c, x)] += from_core[e, chip_part(u, x)]

    def gram_share(e, u):
        chip_copy(e, u).wait_recv()
        gram[e, part_of(u, c, x)] = (
            parts[e, part_of(u, c, x)]
            + from_chip[e, pl.ds(starts[u] // groups, sizes[u] // groups)]
        ).astype(jnp.bfloat16)
        share_copy(e, u, 0).start()
        share_copy(e, u, 1).start()

    def relay(e, u):
        share_copy(e, u, 0).wait_recv()
        share_copy(e, u, 2).start()

    def gram_ready(e, u):
        block = gram.at[e, core_half(u, 1 - c)]
        remote(
            block, block, s_send.at[1], s_recv.at[e, u, 1], {"aa": core_mate}
        ).wait_recv()

    def accumulate(held, e, halves, first, start, count):
        @pl.loop(0, count // half)
        def _(t):
            part = pl.ds(pl.multiple_of(start + t * half, 16), half)
            term = sum(
                jnp.dot(
                    held[e, h, part, :], gram[e, h * wide : (h + 1) * wide, :],
                    preferred_element_type=jnp.float32,
                )
                for h in halves
            )
            if first:
                total[part, :] = term
            else:
                total[part, :] += term

    last = n - 1
    events = [(0, (0,), [(0, u) for u in range(3)])]
    for s in range(1, middle + 1):
        blocks = [2 * s - 1, 2 * s] if s < middle else [last]
        for u, group in enumerate(((0, 1), (2,), (3,))):
            events.append((s, group, [(e, u) for e in blocks]))
    final = len(events) - 1

    def each(do, i):
        if i >= 0:
            for unit in events[i][2]:
                do(*unit)

    def first_power(e):
        for u in range(3):
            gram_ready(e, u)
        accumulate(panel, e, (0, 1), e == 0, 0, rows)

    early = {final - 2: (0, 1, 2), final - 1: (3,), final: (4,)}
    each(gram_partial, 0)
    for i in range(1, final + 1):
        s, group, units = events[i]
        for e in early.get(i, ()):
            first_power(e)
        pass_x(s, group[0])
        if i > 1:
            each(gram_share, i - 1)
        for p in group[1:]:
            pass_x(s, p)
        if i == 1:
            each(core_sum, 0)
        each(gram_partial, i)
        if i == 2:
            each(gram_share, 0)
        if i == 3:
            each(relay, 0)
        if i > 2:
            each(relay, i - 2)
        each(core_sum, i)
    first_power(5)
    first_power(6)
    each(gram_share, final)
    each(relay, final - 1)
    gram_ready(last, 0)
    accumulate(panel, last, (0,), False, 0, rows)
    each(relay, final)
    gram_ready(last, 1)
    gram_ready(last, 2)

    for k in range(2):
        part = pl.ds(k * half, half)
        accumulate(panel, last, (1,), False, k * half, half)
        for h in range(2):
            powers[0, h, part, :] = total[part, h * wide : (h + 1) * wide].astype(jnp.bfloat16)
            for d in range(2):
                hop_p(d, 1, h, k).start()

    accumulate(powers, 0, (0, 1), True, 0, rows)
    for s in range(1, middle):
        for k in range(2):
            for h in range(2):
                for d in range(2):
                    pass_p(d, s, h, k)
        for e in (2 * s - 1, 2 * s):
            accumulate(powers, e, (0, 1), False, 0, rows)

    rate = step_ref[()] * factor
    for k in range(2):
        for d in range(2):
            pass_p(d, middle, d, k)
        accumulate(powers, last, (0, 1), False, k * half, half)
        part = pl.ds(k * half, half)
        for h in range(2):
            columns = slice(h * wide, (h + 1) * wide)
            direction = (
                3.4445 * panel[0, h, part, :].astype(jnp.float32)
                - 4.775 * powers[0, h, part, :].astype(jnp.float32)
                + 2.0315 * total[part, columns]
            )
            weight[part, columns] = weight[part, columns] - rate * direction

    def sent(block, send):
        remote(block, block, send, x_recv.at[0, 0, 0], {"aa": core_mate}).wait_send()

    sent(panel.at[pl.ds(1, n - 1)], x_send)
    sent(powers.at[pl.ds(1, n - 1)], y_send)
    sent(from_core, c_send)
    sent(from_chip, p_send)
    for step in range(3):
        sent(gram.at[pl.ds(0, n // groups)], s_send.at[step])
    for kind in range(3):
        grad_copy(kind).wait_send()
    sent(line.at[pl.ds(0, layers - 1)], t_send.at[0])
    sent(line.at[pl.ds(0, 2)], t_send.at[1])
    sent(line.at[0], t_send.at[2])

    @pl.when(c == 1)
    def _():
        sent(line.at[pl.ds(0, 2)], t_send.at[3])
        sent(line.at[pl.ds(0, 2)], t_send.at[4])

    for layer in range(layers):
        for side in range(2):
            from_here = layer <= z if side == 0 else layer >= z

            @pl.when(from_here & can_go[side])
            def _():
                sent(line.at[layer], z_send.at[side, layer])


def fused_step(activations, out_grad, momentum, weight, norm_scale, step_size, n, groups):
    tokens, features = activations.shape
    rows, width = momentum.shape
    wide, middle = width // 2, n // 2
    pieces = 3 if features % 48 == 0 else 1
    dma = pltpu.SemaphoreType.DMA
    vmem = pl.BlockSpec(memory_space=pltpu.VMEM)
    hbm = pl.BlockSpec(memory_space=pltpu.HBM)
    smem = pl.BlockSpec(memory_space=pltpu.SMEM)
    units = dma((n, 3))
    return pl.pallas_call(
        functools.partial(step_kernel, n, groups, 0.2 * math.sqrt(max(ROWS, COLS))),
        out_shape=(
            jax.ShapeDtypeStruct((rows, width), jnp.float32),
            jax.ShapeDtypeStruct((rows, width), jnp.float32),
        ),
        in_specs=[hbm, hbm, hbm, hbm, smem, smem],
        out_specs=(vmem, vmem),
        scratch_shapes=[
            pltpu.VMEM((n // 2, features, tokens), jnp.bfloat16),
            pltpu.VMEM((2, features, tokens), jnp.bfloat16),
            pltpu.VMEM((2, groups, features, tokens), jnp.bfloat16),
            pltpu.VMEM((groups, tokens, width), jnp.bfloat16),
            pltpu.VMEM((n, 2, rows, wide), jnp.bfloat16),
            pltpu.VMEM((n, 2, rows, wide), jnp.bfloat16),
            pltpu.VMEM((n, width, width), jnp.bfloat16),
            pltpu.VMEM((n, width, width), jnp.float32),
            pltpu.VMEM((n, width // 2, width), jnp.float32),
            pltpu.VMEM((n, width // groups, width), jnp.float32),
            pltpu.VMEM((rows, width), jnp.float32),
            dma((2, n // 2)), dma((n // 2, pieces)),
            dma((5,)), dma((2, groups, pieces)), dma((2, pieces)),
            dma((3,)), dma((3,)),
            dma, dma((2, middle, 4)), dma, dma((2, middle, 2, 2)),
            dma, units, dma, units,
            dma((3,)), dma((n, 3, 2)),
            dma((4,)),
        ],
        compiler_params=pltpu.CompilerParams(
            collective_id=0, has_side_effects=True, vmem_limit_bytes=48 * 1024 * 1024
        ),
        name="step",
    )(
        pltpu.with_memory_space_constraint(activations.T, pltpu.HBM),
        pltpu.with_memory_space_constraint(out_grad, pltpu.HBM), momentum, weight, norm_scale, step_size)


def plain_gradient(activations, out_grad):
    features = lax.all_to_all(
        lax.all_gather(activations, "ba", axis=1, tiled=True),
        "aa", split_axis=1, concat_axis=0, tiled=True,
    )
    return inner_rows(features, lax.all_gather(out_grad, "aa", axis=0, tiled=True))


def plain_direction(scaled):
    row_panel = lax.all_gather(scaled, "ba", axis=1, tiled=True)
    gram_part = inner_rows(row_panel, scaled)
    width = gram_part.shape[0]
    groups = lax.axis_size("aa")
    padding = (groups - width % groups) % groups
    padded = jnp.pad(gram_part, ((0, padding), (0, 0)))
    share = lax.psum_scatter(padded, "aa", scatter_dimension=0, tiled=True).astype(jnp.bfloat16)
    gram_cols = lax.all_gather(share, "aa", axis=0, tiled=True)[:width]
    first_power = jnp.dot(row_panel, gram_cols, preferred_element_type=jnp.float32).astype(
        jnp.bfloat16
    )
    second_power = jnp.dot(
        lax.all_gather(first_power, "ba", axis=1, tiled=True),
        gram_cols,
        preferred_element_type=jnp.float32,
    )
    return (
        3.4445 * scaled.astype(jnp.float32)
        - 4.775 * first_power.astype(jnp.float32)
        + 2.0315 * second_power
    )


def per_device(activations, out_grad, momentum, weight, norm_scale, step_size):
    n, groups = lax.axis_size("ba"), lax.axis_size("aa")
    rows, width = momentum.shape
    tokens, features = activations.shape
    fits = (
        groups == 4 and n == 2 * groups and rows == 2 * features
        and features % 16 == 0 and tokens % 128 == 0 and width % 512 == 0
        and 4 * n * rows * width + 9 * n * width * width + 17 * rows * width < 56 * 2**20
    )
    if fits:
        return fused_step(
            activations, out_grad, momentum, weight, norm_scale, step_size, n, groups
        )
    new_momentum = 0.95 * momentum + plain_gradient(activations, out_grad)
    scaled = (new_momentum / norm_scale).astype(jnp.bfloat16)
    factor = 0.2 * math.sqrt(max(ROWS, COLS))
    new_weight = weight - step_size * factor * plain_direction(scaled)
    return (new_weight, new_momentum)


def solution(mesh):
    placed = (P("aa", "ba"), P("aa", "ba"), P("aa", "ba"), P("aa", "ba"), P(), P())
    return jax.shard_map(
        per_device,
        mesh=mesh,
        in_specs=placed,
        out_specs=(P("aa", "ba"), P("aa", "ba")),
        check_vma=False,
    )
```

```python
import functools
import math

import jax
import jax.numpy as jnp
from jax import lax
from jax.experimental import pallas as pl
from jax.experimental.pallas import tpu as pltpu
from jax.sharding import PartitionSpec as P

ROWS = 4224
COLS = 4096
MESH = pl.DeviceIdType.MESH


def inner_rows(left, right):
    return lax.dot_general(
        left, right, (((0,), (0,)), ((), ())), preferred_element_type=jnp.float32
    )


def step_kernel(
    n, groups, factor,
    act_hbm, grad_hbm, momentum_hbm, weight_hbm, scale_ref, step_ref,
    weight, momentum,
    line, stage, tiles, grads, panel, powers, gram, parts, from_core, from_chip, total,
    z_send, z_recv, t_send, t_recv, b_recv, g_send, g_recv,
    x_send, x_recv, y_send, y_recv, c_send, c_recv, p_send, p_recv, s_send, s_recv,
    load_sem,
):
    half = line.shape[1]
    rows, width = momentum.shape
    wide, middle, layers = width // 2, n // 2, n // 2
    core_rows, share = wide // 2, wide // groups
    pieces = 3 if half % 48 == 0 else 1
    a, b = lax.axis_index("aa"), lax.axis_index("ba")
    x, c, z, y = a // 2, a % 2, b // 2, b % 2
    core_mate = 2 * x + 1 - c
    chip_mate = 2 * (1 - x) + c
    y_mate = 2 * z + 1 - y

    loads = [
        pltpu.make_async_copy(act_hbm, line.at[z], load_sem.at[0]),
        pltpu.make_async_copy(grad_hbm, grads.at[a], load_sem.at[1]),
        pltpu.make_async_copy(momentum_hbm, momentum, load_sem.at[2]),
        pltpu.make_async_copy(weight_hbm, weight, load_sem.at[3]),
    ]
    for load in loads:
        load.start()

    place = z + y * (n - 1 - 2 * z)

    def at(position):
        position = (position + n) % n
        column = position // middle
        return 2 * (position + column * (n - 1 - 2 * position)) + column

    neighbours = (at(place + 1), at(place - 1))

    barrier = pltpu.get_barrier_semaphore()
    for r in range(1, groups):
        pl.semaphore_signal(barrier, 1, device_id={"aa": (a + r) % groups}, device_id_type=MESH)
    for r in range(groups):
        pl.semaphore_signal(
            barrier, 1, device_id={"aa": (a + r) % groups, "ba": y_mate}, device_id_type=MESH
        )

    @pl.when(z > 0)
    def _():
        pl.semaphore_signal(barrier, 1, device_id={"ba": b - 2}, device_id_type=MESH)

    @pl.when(z < layers - 1)
    def _():
        pl.semaphore_signal(barrier, 1, device_id={"ba": b + 2}, device_id_type=MESH)

    sides = (z + layers - 1) // layers + (2 * layers - 2 - z) // layers
    pl.semaphore_wait(barrier, 2 * groups - 1 + sides)

    piece = half // pieces

    def cut(j):
        return pl.ds(j * piece, piece)

    def remote(source, target, send, recv, where):
        return pltpu.make_async_remote_copy(
            src_ref=source, dst_ref=target, send_sem=send, recv_sem=recv,
            device_id=where, device_id_type=MESH,
        )

    def z_hop(layer, side, j):
        block = line.at[layer, cut(j)]
        return remote(
            block, block, z_send.at[side, layer], z_recv.at[layer, j], {"ba": b + 2 - 4 * side}
        )

    def near_copy(layer, j):
        return remote(
            line.at[layer, cut(j)], tiles.at[y, a, cut(j)], t_send.at[0], t_recv.at[y, a, j],
            {"aa": layer},
        )

    def far_copy(layer, j):
        return remote(
            line.at[layer, cut(j)], tiles.at[y, a, cut(j)], t_send.at[1], t_recv.at[y, a, j],
            {"aa": layer, "ba": y_mate},
        )

    def relay_copy(j):
        block = tiles.at[y, 2 * (1 - x), cut(j)]
        return remote(block, block, t_send.at[2], t_recv.at[y, 2 * (1 - x), j], {"ba": y_mate})

    def side_copy(layer, j):
        return remote(
            line.at[layer, cut(j)], stage.at[layer % 2, cut(j)], t_send.at[3],
            b_recv.at[layer % 2, j], {"ba": y_mate},
        )

    def cross_copy(slot, j):
        return remote(
            stage.at[slot, cut(j)], tiles.at[1 - y, a, cut(j)], t_send.at[4],
            t_recv.at[1 - y, a, j], {"aa": 2 * (1 - x) + slot},
        )

    def tile_arrival(k, r, j):
        block = tiles.at[k, r, cut(j)]
        return remote(block, block, t_send.at[0], t_recv.at[k, r, j], {"aa": core_mate})

    def deliver(layer, j):
        pl.when(layer // 2 == x)(far_copy(layer, j).start)
        pl.when((layer // 2 != x) & (c == 1))(side_copy(layer, j).start)
        pl.when(layer != a)(near_copy(layer, j).start)

        @pl.when(layer == a)
        def _():
            tiles[y, a, cut(j)] = line[layer, cut(j)]

    def grad_copy(kind):
        slot = chip_mate if kind == 2 else a
        return remote(
            grads.at[slot], grads.at[slot], g_send.at[kind], g_recv.at[kind],
            {"aa": chip_mate if kind == 0 else core_mate},
        )

    loads[0].wait()
    loads[1].wait()
    can_go = (z < layers - 1, z > 0)
    for j in range(pieces):
        for side in range(2):
            pl.when(can_go[side])(z_hop(z, side, j).start)
        deliver(z, j)
        if j == 0:
            grad_copy(0).start()
            grad_copy(1).start()
    for distance in range(1, layers + 1):
        if distance < layers:
            for j in range(pieces):
                for side in range(2):
                    layer = z - distance if side == 0 else z + distance

                    @pl.when((layer >= 0) & (layer < layers))
                    def _():
                        z_hop(layer, side, j).wait_recv()
                        pl.when(can_go[side])(z_hop(layer, side, j).start)
                        deliver(layer, j)

        for side in range(2):
            layer = z - distance + 1 if side == 0 else z + distance - 1
            there = (layer >= 0) & (layer < layers) & ((side == 0) | (distance > 1))

            @pl.when(there & (layer // 2 != x) & (c == 1))
            def _():
                for j in range(pieces):
                    side_copy(layer, j).wait_recv()
                    cross_copy(layer % 2, j).start()

        @pl.when((z - a == distance - 1) | (a - z == distance - 1))
        def _():
            for j in range(pieces):
                tile_arrival(y, 2 * (1 - x), j).wait_recv()
                relay_copy(j).start()

        if distance == 1:
            grad_copy(0).wait_recv()
            grad_copy(2).start()
    grad_copy(1).wait_recv()
    grad_copy(2).wait_recv()
    loads[2].wait()
    loads[3].wait()

    by_columns = [(h, k) for h in range(2) for k in range(2)]

    def row_half(position, k):
        position = (position + n) % n
        return pl.ds(pl.multiple_of((position // middle + k) % 2 * half, 16), half)

    def hop(held, send, recv, first, d, s, h, k, arrival=False):
        target = n - 1 if s == middle else 2 * s - 1 + d
        origin = 0 if s == 1 else 2 * s - 3 + d
        steps_back = s if arrival else s - 1
        part = row_half(place - steps_back + 2 * d * steps_back, k) if first else pl.ds(k * half, half)
        return remote(
            held.at[origin, h, part], held.at[target, h, part], send, recv.at[d, s - 1, h, k],
            {"ba": neighbours[d]},
        )

    def goes(first, d, s, h, k):
        return s < middle or d == (k if first else h)

    def pass_on(held, send, recv, first, d, s, h, k):
        hop(held, send, recv, first, d, s, h, k, arrival=True).wait_recv()
        if s < middle and goes(first, d, s + 1, h, k):
            hop(held, send, recv, first, d, s + 1, h, k).start()

    ring_x = (panel, x_send, x_recv, True)
    for k in range(2):
        owner = y if k == 0 else 1 - y
        for r in range(groups):
            @pl.when((r != 2 * (1 - x)) & (r != a) if k == 0 else r >= 0)
            def _():
                for j in range(pieces):
                    tile_arrival(owner, r, j).wait_recv()

        @pl.loop(0, pieces)
        def _(t):
            source = pl.ds(pl.multiple_of(t * piece, 16), piece)
            part = pl.ds(pl.multiple_of(owner * half + t * piece, 16), piece)
            gradient = sum(
                jnp.dot(tiles[owner, r, source, :], grads[r], preferred_element_type=jnp.float32)
                for r in range(groups)
            )
            updated = 0.95 * momentum[part, :] + gradient
            momentum[part, :] = updated
            scaled = (updated / scale_ref[()]).astype(jnp.bfloat16)
            for h in range(2):
                panel[0, h, part, :] = scaled[:, h * wide : (h + 1) * wide]

        if k == 0:
            for d in range(2):
                hop(*ring_x, d, 1, 0, 0).start()

    for h, k in by_columns[1:]:
        for d in range(2):
            hop(*ring_x, d, 1, h, k).start()

    def span(start, size):
        return pl.ds(pl.multiple_of(start, size), size)

    mine, theirs = c * core_rows + x * share, c * core_rows + (1 - x) * share

    last = n - 1
    halved = [(last - 2, 1), (last - 1, 1), (last, 0), (last, 1)]

    def slot(e, h, q):
        return (n + halved.index((e, h)) // 2, halved.index((e, h)) % 2) if q == 1 else (e, h)

    def columns_of(q):
        return pl.ds(0, width) if q is None else pl.ds(q * wide, wide)

    def core_copy(e, h, q):
        return remote(
            parts.at[e, h, span((1 - c) * core_rows, core_rows), columns_of(q)],
            from_core.at[e, h, :, columns_of(q)],
            c_send, c_recv.at[slot(e, h, q)], {"aa": core_mate},
        )

    def chip_copy(e, h, q):
        return remote(
            parts.at[e, h, span(theirs, share), columns_of(q)], from_chip.at[e, h, :, columns_of(q)],
            p_send, p_recv.at[slot(e, h, q)], {"aa": chip_mate},
        )

    def share_copy(e, h, q, step):
        block = gram.at[
            e, span(h * wide + (theirs if step == 2 else mine), share), columns_of(q)
        ]
        return remote(
            block, block, s_send.at[step], s_recv.at[(*slot(e, h, q), min(step, 1))],
            {"aa": chip_mate if step == 0 else core_mate},
        )

    def gram_partial(e, h, q):
        if q is None:
            @pl.loop(0, 2)
            def _(r):
                parts[e, h, :, span(r * wide, wide)] = inner_rows(panel[e, h], panel[0, r])
        else:
            parts[e, h, :, columns_of(q)] = inner_rows(panel[e, h], panel[0, q])
        core_copy(e, h, q).start()

    def core_sum(e, h, q):
        columns = columns_of(q)
        core_copy(e, h, q).wait_recv()
        parts[e, h, span(theirs, share), columns] += (
            from_core[e, h, span((1 - x) * share, share), columns]
        )
        chip_copy(e, h, q).start()
        parts[e, h, span(mine, share), columns] += from_core[e, h, span(x * share, share), columns]

    def gram_share(e, h, q):
        columns = columns_of(q)
        chip_copy(e, h, q).wait_recv()
        gram[e, span(h * wide + mine, share), columns] = (
            parts[e, h, span(mine, share), columns] + from_chip[e, h, :, columns]
        ).astype(jnp.bfloat16)
        share_copy(e, h, q, 0).start()
        share_copy(e, h, q, 1).start()

    def relay(e, h, q):
        share_copy(e, h, q, 0).wait_recv()
        share_copy(e, h, q, 2).start()

    def gram_ready(e, h, q):
        block = gram.at[e, span(h * wide + (1 - c) * core_rows, core_rows), columns_of(q)]
        remote(
            block, block, s_send.at[1], s_recv.at[(*slot(e, h, q), 1)], {"aa": core_mate}
        ).wait_recv()

    def accumulate(held, e, halves, first, start, count):
        @pl.loop(0, count // half)
        def _(t):
            part = pl.ds(pl.multiple_of(start + t * half, 16), half)
            term = sum(
                jnp.dot(
                    held[e, h, part, :], gram[e, h * wide : (h + 1) * wide, :],
                    preferred_element_type=jnp.float32,
                )
                for h in halves
            )
            if first:
                total[part, :] = term
            else:
                total[part, :] += term

    whole = [[(0, h, None) for h in range(2)]]
    for s in range(1, middle - 1):
        for h in range(2):
            whole.append([(e, h, None) for e in (2 * s - 1, 2 * s)])
    whole.append([(e, 0, None) for e in (last - 2, last - 1)])
    near, mid, end = (
        [[(e, h, q) for e, h in group] for q in range(2)]
        for group in (halved[:2], halved[2:3], halved[3:])
    )

    def each(do, units):
        for unit in units:
            do(*unit)

    def first_power(e):
        for h in range(2):
            gram_ready(e, h, None)
        accumulate(panel, e, (0, 1), e == 0, 0, rows)

    def add_columns(e, halves, q):
        columns = slice(q * wide, (q + 1) * wide)
        for k in range(2):
            part = pl.ds(k * half, half)
            total[part, columns] += sum(
                jnp.dot(
                    panel[e, h, part, :], gram[e, h * wide : (h + 1) * wide, columns],
                    preferred_element_type=jnp.float32,
                )
                for h in halves
            )

    def receive(s, h, k):
        for d in range(2):
            if goes(True, d, s, h, k):
                pass_on(*ring_x, d, s, h, k)

    def send_power(q):
        columns = slice(q * wide, (q + 1) * wide)
        for k in range(2):
            part = pl.ds(k * half, half)
            first_powers = total[part, columns] + jnp.dot(
                panel[last, 1, part, :], gram[last, wide:, columns],
                preferred_element_type=jnp.float32,
            )
            powers[0, q, part, :] = first_powers.astype(jnp.bfloat16)
            for d in range(2):
                hop(*ring_p, d, 1, q, k).start()

    ring_p = (powers, y_send, y_recv, False)
    each(gram_partial, whole[0])
    for i in range(1, len(whole)):
        s, h = (i + 1) // 2, (i + 1) % 2
        receive(s, h, 0)
        if i > 1:
            each(gram_share, whole[i - 1])
        receive(s, h, 1)
        if i == 1:
            each(core_sum, whole[0])
        each(gram_partial, whole[i])
        if i == 2:
            each(gram_share, whole[0])
        each(core_sum, whole[i])
        if i == 3:
            each(relay, whole[0])
        if i > 1:
            each(relay, whole[i - 1])

    receive(middle - 1, 1, 0)
    each(gram_share, whole[-1])
    receive(middle - 1, 1, 1)
    for q in range(2):
        each(gram_partial, near[q])
    for q in range(2):
        each(core_sum, near[q])
    each(relay, whole[-1])
    for e in range(4):
        first_power(e)
    for k in range(2):
        receive(middle, 0, k)
    for q in range(2):
        each(gram_partial, mid[q])
    each(core_sum, mid[0])
    each(gram_share, near[0])
    for k in range(2):
        receive(middle, 1, k)
    for q in range(2):
        each(gram_partial, end[q])
    each(core_sum, end[0])
    each(gram_share, mid[0])
    each(core_sum, mid[1])
    each(relay, near[0])
    first_power(4)
    each(gram_share, end[0])
    each(gram_share, near[1])
    each(core_sum, end[1])
    each(relay, mid[0])
    for e in (last - 2, last - 1):
        gram_ready(e, 0, None)
        gram_ready(e, 1, 0)
        add_columns(e, (0, 1), 0)
    gram_ready(last, 0, 0)
    add_columns(last, (0,), 0)
    each(relay, end[0])
    gram_ready(last, 1, 0)
    send_power(0)
    each(gram_share, mid[1])
    each(relay, near[1])
    each(gram_share, end[1])
    each(relay, mid[1])
    for e in (last - 2, last - 1):
        gram_ready(e, 1, 1)
        add_columns(e, (0, 1), 1)
    gram_ready(last, 0, 1)
    add_columns(last, (0,), 1)
    each(relay, end[1])
    gram_ready(last, 1, 1)
    send_power(1)

    accumulate(powers, 0, (0, 1), True, 0, rows)
    for s in range(1, middle):
        for h, k in by_columns:
            for d in range(2):
                pass_on(*ring_p, d, s, h, k)
        for e in (2 * s - 1, 2 * s):
            accumulate(powers, e, (0, 1), False, 0, rows)

    rate = step_ref[()] * factor
    for k in range(2):
        for d in range(2):
            pass_on(*ring_p, d, middle, d, k)
        accumulate(powers, last, (0, 1), False, k * half, half)
        part = pl.ds(k * half, half)
        for h in range(2):
            columns = slice(h * wide, (h + 1) * wide)
            direction = (
                3.4445 * panel[0, h, part, :].astype(jnp.float32)
                - 4.775 * powers[0, h, part, :].astype(jnp.float32)
                + 2.0315 * total[part, columns]
            )
            weight[part, columns] = weight[part, columns] - rate * direction

    def sent(block, send):
        remote(block, block, send, x_recv.at[0, 0, 0, 0], {"aa": core_mate}).wait_send()

    sent(panel.at[pl.ds(1, n - 1)], x_send)
    sent(powers.at[pl.ds(1, n - 1)], y_send)
    sent(from_core, c_send)
    sent(from_chip, p_send)
    for step in range(3):
        sent(gram.at[pl.ds(0, n // groups)], s_send.at[step])
    for kind in range(3):
        grad_copy(kind).wait_send()
    sent(line.at[pl.ds(0, layers - 1)], t_send.at[0])
    sent(line.at[pl.ds(0, 2)], t_send.at[1])
    sent(line.at[0], t_send.at[2])

    @pl.when(c == 1)
    def _():
        sent(line.at[pl.ds(0, 2)], t_send.at[3])
        sent(line.at[pl.ds(0, 2)], t_send.at[4])

    for layer in range(layers):
        for side in range(2):
            from_here = layer <= z if side == 0 else layer >= z

            @pl.when(from_here & can_go[side])
            def _():
                sent(line.at[layer], z_send.at[side, layer])


def fused_step(activations, out_grad, momentum, weight, norm_scale, step_size, n, groups):
    tokens, features = activations.shape
    rows, width = momentum.shape
    wide, middle = width // 2, n // 2
    pieces = 3 if features % 48 == 0 else 1
    dma = pltpu.SemaphoreType.DMA
    vmem = pl.BlockSpec(memory_space=pltpu.VMEM)
    hbm = pl.BlockSpec(memory_space=pltpu.HBM)
    smem = pl.BlockSpec(memory_space=pltpu.SMEM)
    ring = dma((2, middle, 2, 2))
    units = dma((n + 2, 2))
    return pl.pallas_call(
        functools.partial(step_kernel, n, groups, 0.2 * math.sqrt(max(ROWS, COLS))),
        out_shape=(
            jax.ShapeDtypeStruct((rows, width), jnp.float32),
            jax.ShapeDtypeStruct((rows, width), jnp.float32),
        ),
        in_specs=[hbm, hbm, hbm, hbm, smem, smem],
        out_specs=(vmem, vmem),
        scratch_shapes=[
            pltpu.VMEM((n // 2, features, tokens), jnp.bfloat16),
            pltpu.VMEM((2, features, tokens), jnp.bfloat16),
            pltpu.VMEM((2, groups, features, tokens), jnp.bfloat16),
            pltpu.VMEM((groups, tokens, width), jnp.bfloat16),
            pltpu.VMEM((n, 2, rows, wide), jnp.bfloat16),
            pltpu.VMEM((n, 2, rows, wide), jnp.bfloat16),
            pltpu.VMEM((n, width, width), jnp.bfloat16),
            pltpu.VMEM((n, 2, wide, width), jnp.float32),
            pltpu.VMEM((n, 2, wide // 2, width), jnp.float32),
            pltpu.VMEM((n, 2, wide // groups, width), jnp.float32),
            pltpu.VMEM((rows, width), jnp.float32),
            dma((2, n // 2)), dma((n // 2, pieces)),
            dma((5,)), dma((2, groups, pieces)), dma((2, pieces)),
            dma((3,)), dma((3,)),
            dma, ring, dma, ring,
            dma, units, dma, units,
            dma((3,)), dma((n + 2, 2, 2)),
            dma((4,)),
        ],
        compiler_params=pltpu.CompilerParams(
            collective_id=0, has_side_effects=True, vmem_limit_bytes=48 * 1024 * 1024
        ),
        name="step",
    )(
        pltpu.with_memory_space_constraint(activations.T, pltpu.HBM),
        pltpu.with_memory_space_constraint(out_grad, pltpu.HBM), momentum, weight, norm_scale, step_size)


def plain_gradient(activations, out_grad):
    features = lax.all_to_all(
        lax.all_gather(activations, "ba", axis=1, tiled=True),
        "aa", split_axis=1, concat_axis=0, tiled=True,
    )
    return inner_rows(features, lax.all_gather(out_grad, "aa", axis=0, tiled=True))


def plain_direction(scaled):
    row_panel = lax.all_gather(scaled, "ba", axis=1, tiled=True)
    gram_part = inner_rows(row_panel, scaled)
    width = gram_part.shape[0]
    groups = lax.axis_size("aa")
    padding = (groups - width % groups) % groups
    padded = jnp.pad(gram_part, ((0, padding), (0, 0)))
    share = lax.psum_scatter(padded, "aa", scatter_dimension=0, tiled=True).astype(jnp.bfloat16)
    gram_cols = lax.all_gather(share, "aa", axis=0, tiled=True)[:width]
    first_power = jnp.dot(row_panel, gram_cols, preferred_element_type=jnp.float32).astype(
        jnp.bfloat16
    )
    second_power = jnp.dot(
        lax.all_gather(first_power, "ba", axis=1, tiled=True),
        gram_cols,
        preferred_element_type=jnp.float32,
    )
    return (
        3.4445 * scaled.astype(jnp.float32)
        - 4.775 * first_power.astype(jnp.float32)
        + 2.0315 * second_power
    )


def per_device(activations, out_grad, momentum, weight, norm_scale, step_size):
    n, groups = lax.axis_size("ba"), lax.axis_size("aa")
    rows, width = momentum.shape
    tokens, features = activations.shape
    fits = (
        groups == 4 and n == 2 * groups and rows == 2 * features
        and features % 16 == 0 and tokens % 128 == 0 and width % 256 == 0
        and width % (32 * groups) == 0
        and 4 * n * rows * width + 9 * n * width * width + 17 * rows * width < 56 * 2**20
    )
    if fits:
        return fused_step(
            activations, out_grad, momentum, weight, norm_scale, step_size, n, groups
        )
    new_momentum = 0.95 * momentum + plain_gradient(activations, out_grad)
    scaled = (new_momentum / norm_scale).astype(jnp.bfloat16)
    factor = 0.2 * math.sqrt(max(ROWS, COLS))
    new_weight = weight - step_size * factor * plain_direction(scaled)
    return (new_weight, new_momentum)


def solution(mesh):
    placed = (P("aa", "ba"), P("aa", "ba"), P("aa", "ba"), P("aa", "ba"), P(), P())
    return jax.shard_map(
        per_device,
        mesh=mesh,
        in_specs=placed,
        out_specs=(P("aa", "ba"), P("aa", "ba")),
        check_vma=False,
    )
```

```python
import functools
import math

import jax
import jax.numpy as jnp
from jax import lax
from jax.experimental import pallas as pl
from jax.experimental.pallas import tpu as pltpu
from jax.sharding import PartitionSpec as P

ROWS = 4224
COLS = 4096
MESH = pl.DeviceIdType.MESH


def inner_rows(left, right):
    return lax.dot_general(
        left, right, (((0,), (0,)), ((), ())), preferred_element_type=jnp.float32
    )


def step_kernel(
    n, groups, factor,
    act_hbm, grad_hbm, momentum_hbm, weight_hbm, scale_ref, step_ref,
    weight, momentum,
    line, stage, tiles, grads, panel, powers, gram, parts, from_core, from_chip, total,
    z_send, z_recv, t_send, t_recv, b_recv, g_send, g_recv,
    x_send, x_recv, y_send, y_recv, c_send, c_recv, p_send, p_recv, s_send, s_recv,
    load_sem,
):
    half = line.shape[1]
    rows, width = momentum.shape
    wide, middle, layers = width // 2, n // 2, n // 2
    core_rows, share = wide // 2, wide // groups
    pieces = 3 if half % 48 == 0 else 1
    a, b = lax.axis_index("aa"), lax.axis_index("ba")
    x, c, z, y = a // 2, a % 2, b // 2, b % 2
    core_mate = 2 * x + 1 - c
    chip_mate = 2 * (1 - x) + c
    y_mate = 2 * z + 1 - y

    loads = [
        pltpu.make_async_copy(act_hbm, line.at[z], load_sem.at[0]),
        pltpu.make_async_copy(grad_hbm, grads.at[a], load_sem.at[1]),
        pltpu.make_async_copy(momentum_hbm, momentum, load_sem.at[2]),
        pltpu.make_async_copy(weight_hbm, weight, load_sem.at[3]),
    ]
    for load in loads:
        load.start()

    place = z + y * (n - 1 - 2 * z)

    def at(position):
        position = (position + n) % n
        column = position // middle
        return 2 * (position + column * (n - 1 - 2 * position)) + column

    neighbours = (at(place + 1), at(place - 1))

    barrier = pltpu.get_barrier_semaphore()
    for r in range(1, groups):
        pl.semaphore_signal(barrier, 1, device_id={"aa": (a + r) % groups}, device_id_type=MESH)
    for r in range(groups):
        pl.semaphore_signal(
            barrier, 1, device_id={"aa": (a + r) % groups, "ba": y_mate}, device_id_type=MESH
        )

    @pl.when(z > 0)
    def _():
        pl.semaphore_signal(barrier, 1, device_id={"ba": b - 2}, device_id_type=MESH)

    @pl.when(z < layers - 1)
    def _():
        pl.semaphore_signal(barrier, 1, device_id={"ba": b + 2}, device_id_type=MESH)

    sides = (z + layers - 1) // layers + (2 * layers - 2 - z) // layers
    pl.semaphore_wait(barrier, 2 * groups - 1 + sides)

    piece = half // pieces

    def cut(j):
        return pl.ds(j * piece, piece)

    def remote(source, target, send, recv, where):
        return pltpu.make_async_remote_copy(
            src_ref=source, dst_ref=target, send_sem=send, recv_sem=recv,
            device_id=where, device_id_type=MESH,
        )

    def z_hop(layer, side, j):
        block = line.at[layer, cut(j)]
        return remote(
            block, block, z_send.at[side, layer], z_recv.at[layer, j], {"ba": b + 2 - 4 * side}
        )

    def near_copy(layer, j):
        return remote(
            line.at[layer, cut(j)], tiles.at[y, a, cut(j)], t_send.at[0], t_recv.at[y, a, j],
            {"aa": layer},
        )

    def far_copy(layer, j):
        return remote(
            line.at[layer, cut(j)], tiles.at[y, a, cut(j)], t_send.at[1], t_recv.at[y, a, j],
            {"aa": layer, "ba": y_mate},
        )

    def relay_copy(j):
        block = tiles.at[y, 2 * (1 - x), cut(j)]
        return remote(block, block, t_send.at[2], t_recv.at[y, 2 * (1 - x), j], {"ba": y_mate})

    def side_copy(layer, j):
        return remote(
            line.at[layer, cut(j)], stage.at[layer % 2, cut(j)], t_send.at[3],
            b_recv.at[layer % 2, j], {"ba": y_mate},
        )

    def cross_copy(slot, j):
        return remote(
            stage.at[slot, cut(j)], tiles.at[1 - y, a, cut(j)], t_send.at[4],
            t_recv.at[1 - y, a, j], {"aa": 2 * (1 - x) + slot},
        )

    def tile_arrival(k, r, j):
        block = tiles.at[k, r, cut(j)]
        return remote(block, block, t_send.at[0], t_recv.at[k, r, j], {"aa": core_mate})

    def deliver(layer, j):
        pl.when(layer // 2 == x)(far_copy(layer, j).start)
        pl.when((layer // 2 != x) & (c == 1))(side_copy(layer, j).start)
        pl.when(layer != a)(near_copy(layer, j).start)

        @pl.when(layer == a)
        def _():
            tiles[y, a, cut(j)] = line[layer, cut(j)]

    def grad_copy(kind):
        slot = chip_mate if kind == 2 else a
        return remote(
            grads.at[slot], grads.at[slot], g_send.at[kind], g_recv.at[kind],
            {"aa": chip_mate if kind == 0 else core_mate},
        )

    loads[0].wait()
    loads[1].wait()
    can_go = (z < layers - 1, z > 0)
    for j in range(pieces):
        for side in range(2):
            pl.when(can_go[side])(z_hop(z, side, j).start)
        deliver(z, j)
        if j == 0:
            grad_copy(0).start()
            grad_copy(1).start()
    for distance in range(1, layers + 1):
        if distance < layers:
            for j in range(pieces):
                for side in range(2):
                    layer = z - distance if side == 0 else z + distance

                    @pl.when((layer >= 0) & (layer < layers))
                    def _():
                        z_hop(layer, side, j).wait_recv()
                        pl.when(can_go[side])(z_hop(layer, side, j).start)
                        deliver(layer, j)

        for side in range(2):
            layer = z - distance + 1 if side == 0 else z + distance - 1
            there = (layer >= 0) & (layer < layers) & ((side == 0) | (distance > 1))

            @pl.when(there & (layer // 2 != x) & (c == 1))
            def _():
                for j in range(pieces):
                    side_copy(layer, j).wait_recv()
                    cross_copy(layer % 2, j).start()

        @pl.when((z - a == distance - 1) | (a - z == distance - 1))
        def _():
            for j in range(pieces):
                tile_arrival(y, 2 * (1 - x), j).wait_recv()
                relay_copy(j).start()

        if distance == 1:
            grad_copy(0).wait_recv()
            grad_copy(2).start()
    grad_copy(1).wait_recv()
    grad_copy(2).wait_recv()
    loads[2].wait()
    loads[3].wait()

    by_columns = [(h, k) for h in range(2) for k in range(2)]

    def row_half(position, k):
        position = (position + n) % n
        return pl.ds(pl.multiple_of((position // middle + k) % 2 * half, 16), half)

    def hop(held, send, recv, first, d, s, h, k, arrival=False):
        target = n - 1 if s == middle else 2 * s - 1 + d
        origin = 0 if s == 1 else 2 * s - 3 + d
        steps_back = s if arrival else s - 1
        part = row_half(place - steps_back + 2 * d * steps_back, k) if first else pl.ds(k * half, half)
        return remote(
            held.at[origin, h, part], held.at[target, h, part], send, recv.at[d, s - 1, h, k],
            {"ba": neighbours[d]},
        )

    def goes(first, d, s, h, k):
        return s < middle or d == (k if first else h)

    def pass_on(held, send, recv, first, d, s, h, k):
        hop(held, send, recv, first, d, s, h, k, arrival=True).wait_recv()
        if s < middle and goes(first, d, s + 1, h, k):
            hop(held, send, recv, first, d, s + 1, h, k).start()

    ring_x = (panel, x_send, x_recv, True)
    for k in range(2):
        owner = y if k == 0 else 1 - y
        for r in range(groups):
            @pl.when((r != 2 * (1 - x)) & (r != a) if k == 0 else r >= 0)
            def _():
                for j in range(pieces):
                    tile_arrival(owner, r, j).wait_recv()

        @pl.loop(0, pieces)
        def _(t):
            source = pl.ds(pl.multiple_of(t * piece, 16), piece)
            part = pl.ds(pl.multiple_of(owner * half + t * piece, 16), piece)
            gradient = sum(
                jnp.dot(tiles[owner, r, source, :], grads[r], preferred_element_type=jnp.float32)
                for r in range(groups)
            )
            updated = 0.95 * momentum[part, :] + gradient
            momentum[part, :] = updated
            scaled = (updated / scale_ref[()]).astype(jnp.bfloat16)
            for h in range(2):
                panel[0, h, part, :] = scaled[:, h * wide : (h + 1) * wide]

        if k == 0:
            for d in range(2):
                hop(*ring_x, d, 1, 0, 0).start()

    for h, k in by_columns[1:]:
        for d in range(2):
            hop(*ring_x, d, 1, h, k).start()

    def span(start, size):
        return pl.ds(pl.multiple_of(start, size), size)

    mine, theirs = c * core_rows + x * share, c * core_rows + (1 - x) * share

    last = n - 1
    halved = [(last - 2, 1), (last - 1, 1), (last, 0), (last, 1)]

    def slot(e, h, q):
        return (n + halved.index((e, h)) // 2, halved.index((e, h)) % 2) if q == 1 else (e, h)

    def columns_of(q):
        return pl.ds(0, width) if q is None else pl.ds(q * wide, wide)

    def core_copy(e, h, q):
        return remote(
            parts.at[e, h, span((1 - c) * core_rows, core_rows), columns_of(q)],
            from_core.at[e, h, :, columns_of(q)],
            c_send, c_recv.at[slot(e, h, q)], {"aa": core_mate},
        )

    def chip_copy(e, h, q):
        return remote(
            parts.at[e, h, span(theirs, share), columns_of(q)], from_chip.at[e, h, :, columns_of(q)],
            p_send, p_recv.at[slot(e, h, q)], {"aa": chip_mate},
        )

    def share_copy(e, h, q, step):
        block = gram.at[
            e, span(h * wide + (theirs if step == 2 else mine), share), columns_of(q)
        ]
        return remote(
            block, block, s_send.at[step], s_recv.at[(*slot(e, h, q), min(step, 1))],
            {"aa": chip_mate if step == 0 else core_mate},
        )

    def gram_partial(e, h, q):
        if q is None:
            @pl.loop(0, 2)
            def _(r):
                parts[e, h, :, span(r * wide, wide)] = inner_rows(panel[e, h], panel[0, r])
        else:
            parts[e, h, :, columns_of(q)] = inner_rows(panel[e, h], panel[0, q])
        core_copy(e, h, q).start()

    def core_sum(e, h, q):
        columns = columns_of(q)
        core_copy(e, h, q).wait_recv()
        parts[e, h, span(theirs, share), columns] += (
            from_core[e, h, span((1 - x) * share, share), columns]
        )
        chip_copy(e, h, q).start()
        parts[e, h, span(mine, share), columns] += from_core[e, h, span(x * share, share), columns]

    def gram_share(e, h, q):
        columns = columns_of(q)
        chip_copy(e, h, q).wait_recv()
        gram[e, span(h * wide + mine, share), columns] = (
            parts[e, h, span(mine, share), columns] + from_chip[e, h, :, columns]
        ).astype(jnp.bfloat16)
        share_copy(e, h, q, 0).start()
        share_copy(e, h, q, 1).start()

    def relay(e, h, q):
        share_copy(e, h, q, 0).wait_recv()
        share_copy(e, h, q, 2).start()

    def gram_ready(e, h, q):
        block = gram.at[e, span(h * wide + (1 - c) * core_rows, core_rows), columns_of(q)]
        remote(
            block, block, s_send.at[1], s_recv.at[(*slot(e, h, q), 1)], {"aa": core_mate}
        ).wait_recv()

    def accumulate(held, e, halves, first, start, count):
        @pl.loop(0, count // half)
        def _(t):
            part = pl.ds(pl.multiple_of(start + t * half, 16), half)
            term = sum(
                jnp.dot(
                    held[e, h, part, :], gram[e, h * wide : (h + 1) * wide, :],
                    preferred_element_type=jnp.float32,
                )
                for h in halves
            )
            if first:
                total[part, :] = term
            else:
                total[part, :] += term

    whole = [[(0, h, None) for h in range(2)]]
    for s in range(1, middle - 1):
        for h in range(2):
            whole.append([(e, h, None) for e in (2 * s - 1, 2 * s)])
    whole.append([(e, 0, None) for e in (last - 2, last - 1)])
    near, mid, end = (
        [[(e, h, q) for e, h in group] for q in range(2)]
        for group in (halved[:2], halved[2:3], halved[3:])
    )

    def each(do, units):
        for unit in units:
            do(*unit)

    def first_power(e):
        for h in range(2):
            gram_ready(e, h, None)
        accumulate(panel, e, (0, 1), e == 0, 0, rows)

    def add_columns(e, halves, q):
        columns = slice(q * wide, (q + 1) * wide)
        for k in range(2):
            part = pl.ds(k * half, half)
            total[part, columns] += sum(
                jnp.dot(
                    panel[e, h, part, :], gram[e, h * wide : (h + 1) * wide, columns],
                    preferred_element_type=jnp.float32,
                )
                for h in halves
            )

    def receive(s, h, k):
        for d in range(2):
            if goes(True, d, s, h, k):
                pass_on(*ring_x, d, s, h, k)

    def send_power(q):
        columns = slice(q * wide, (q + 1) * wide)
        for k in range(2):
            part = pl.ds(k * half, half)
            first_powers = total[part, columns] + jnp.dot(
                panel[last, 1, part, :], gram[last, wide:, columns],
                preferred_element_type=jnp.float32,
            )
            powers[0, q, part, :] = first_powers.astype(jnp.bfloat16)
            for d in range(2):
                hop(*ring_p, d, 1, q, k).start()

    ring_p = (powers, y_send, y_recv, False)
    each(gram_partial, whole[0])
    for i in range(1, len(whole)):
        s, h = (i + 1) // 2, (i + 1) % 2
        receive(s, h, 0)
        if i > 1:
            each(gram_share, whole[i - 1])
        receive(s, h, 1)
        if i == 1:
            each(core_sum, whole[0])
        each(gram_partial, whole[i])
        if i == 2:
            each(gram_share, whole[0])
        each(core_sum, whole[i])
        if i == 3:
            each(relay, whole[0])
        if i > 1:
            each(relay, whole[i - 1])

    receive(middle - 1, 1, 0)
    each(gram_share, whole[-1])
    receive(middle - 1, 1, 1)
    for q in range(2):
        each(gram_partial, near[q])
    for q in range(2):
        each(core_sum, near[q])
    each(relay, whole[-1])
    for e in range(4):
        first_power(e)
    for k in range(2):
        receive(middle, 0, k)
    for q in range(2):
        each(gram_partial, mid[q])
    each(core_sum, mid[0])
    each(gram_share, near[0])
    for k in range(2):
        receive(middle, 1, k)
    for q in range(2):
        each(gram_partial, end[q])
    each(core_sum, end[0])
    each(gram_share, mid[0])
    each(core_sum, mid[1])
    each(relay, near[0])
    first_power(4)
    each(gram_share, end[0])
    each(gram_share, near[1])
    each(core_sum, end[1])
    each(relay, mid[0])
    for e in (last - 2, last - 1):
        gram_ready(e, 0, None)
        gram_ready(e, 1, 0)
        add_columns(e, (0, 1), 0)
    gram_ready(last, 0, 0)
    add_columns(last, (0,), 0)
    each(relay, end[0])
    gram_ready(last, 1, 0)
    send_power(0)
    each(gram_share, mid[1])
    each(relay, near[1])
    each(gram_share, end[1])
    each(relay, mid[1])
    for e in (last - 2, last - 1):
        gram_ready(e, 1, 1)
        add_columns(e, (0, 1), 1)
    gram_ready(last, 0, 1)
    add_columns(last, (0,), 1)
    each(relay, end[1])
    gram_ready(last, 1, 1)
    send_power(1)

    accumulate(powers, 0, (0, 1), True, 0, rows)
    for s in range(1, middle):
        for h, k in by_columns:
            for d in range(2):
                pass_on(*ring_p, d, s, h, k)
        for e in (2 * s - 1, 2 * s):
            accumulate(powers, e, (0, 1), False, 0, rows)

    rate = step_ref[()] * factor
    for k in range(2):
        for d in range(2):
            pass_on(*ring_p, d, middle, d, k)
        accumulate(powers, last, (0, 1), False, k * half, half)
        part = pl.ds(k * half, half)
        for h in range(2):
            columns = slice(h * wide, (h + 1) * wide)
            direction = (
                3.4445 * panel[0, h, part, :].astype(jnp.float32)
                - 4.775 * powers[0, h, part, :].astype(jnp.float32)
                + 2.0315 * total[part, columns]
            )
            weight[part, columns] = weight[part, columns] - rate * direction

    def sent(block, send):
        remote(block, block, send, x_recv.at[0, 0, 0, 0], {"aa": core_mate}).wait_send()

    sent(panel.at[pl.ds(1, n - 1)], x_send)
    sent(powers.at[pl.ds(1, n - 1)], y_send)
    sent(from_core, c_send)
    sent(from_chip, p_send)
    for step in range(3):
        sent(gram.at[pl.ds(0, n // groups)], s_send.at[step])
    for kind in range(3):
        grad_copy(kind).wait_send()
    sent(line.at[pl.ds(0, layers - 1)], t_send.at[0])
    sent(line.at[pl.ds(0, 2)], t_send.at[1])
    sent(line.at[0], t_send.at[2])

    @pl.when(c == 1)
    def _():
        sent(line.at[pl.ds(0, 2)], t_send.at[3])
        sent(line.at[pl.ds(0, 2)], t_send.at[4])

    for layer in range(layers):
        for side in range(2):
            from_here = layer <= z if side == 0 else layer >= z

            @pl.when(from_here & can_go[side])
            def _():
                sent(line.at[layer], z_send.at[side, layer])


def store_kernel(weight, momentum, new_weight, new_momentum, sem):
    copies = [
        pltpu.make_async_copy(weight, new_weight, sem.at[0]),
        pltpu.make_async_copy(momentum, new_momentum, sem.at[1]),
    ]
    for copy in copies:
        copy.start()
    for copy in copies:
        copy.wait()


def fused_step(activations, out_grad, momentum, weight, norm_scale, step_size, n, groups):
    tokens, features = activations.shape
    rows, width = momentum.shape
    wide, middle = width // 2, n // 2
    pieces = 3 if features % 48 == 0 else 1
    dma = pltpu.SemaphoreType.DMA
    vmem = pl.BlockSpec(memory_space=pltpu.VMEM)
    hbm = pl.BlockSpec(memory_space=pltpu.HBM)
    smem = pl.BlockSpec(memory_space=pltpu.SMEM)
    ring = dma((2, middle, 2, 2))
    units = dma((n + 2, 2))
    results = pl.pallas_call(
        functools.partial(step_kernel, n, groups, 0.2 * math.sqrt(max(ROWS, COLS))),
        out_shape=(
            jax.ShapeDtypeStruct((rows, width), jnp.float32),
            jax.ShapeDtypeStruct((rows, width), jnp.float32),
        ),
        in_specs=[hbm, hbm, hbm, hbm, smem, smem],
        out_specs=(vmem, vmem),
        scratch_shapes=[
            pltpu.VMEM((n // 2, features, tokens), jnp.bfloat16),
            pltpu.VMEM((2, features, tokens), jnp.bfloat16),
            pltpu.VMEM((2, groups, features, tokens), jnp.bfloat16),
            pltpu.VMEM((groups, tokens, width), jnp.bfloat16),
            pltpu.VMEM((n, 2, rows, wide), jnp.bfloat16),
            pltpu.VMEM((n, 2, rows, wide), jnp.bfloat16),
            pltpu.VMEM((n, width, width), jnp.bfloat16),
            pltpu.VMEM((n, 2, wide, width), jnp.float32),
            pltpu.VMEM((n, 2, wide // 2, width), jnp.float32),
            pltpu.VMEM((n, 2, wide // groups, width), jnp.float32),
            pltpu.VMEM((rows, width), jnp.float32),
            dma((2, n // 2)), dma((n // 2, pieces)),
            dma((5,)), dma((2, groups, pieces)), dma((2, pieces)),
            dma((3,)), dma((3,)),
            dma, ring, dma, ring,
            dma, units, dma, units,
            dma((3,)), dma((n + 2, 2, 2)),
            dma((4,)),
        ],
        compiler_params=pltpu.CompilerParams(
            collective_id=0, has_side_effects=True, vmem_limit_bytes=48 * 1024 * 1024
        ),
        name="step",
    )(
        pltpu.with_memory_space_constraint(activations.T, pltpu.HBM),
        pltpu.with_memory_space_constraint(out_grad, pltpu.HBM), momentum, weight, norm_scale, step_size)
    return pl.pallas_call(
        store_kernel,
        out_shape=(
            jax.ShapeDtypeStruct((rows, width), jnp.float32),
            jax.ShapeDtypeStruct((rows, width), jnp.float32),
        ),
        in_specs=[vmem, vmem],
        out_specs=(hbm, hbm),
        scratch_shapes=[dma((2,))],
        compiler_params=pltpu.CompilerParams(vmem_limit_bytes=8 * 1024 * 1024),
        name="store",
    )(*results)


def plain_gradient(activations, out_grad):
    features = lax.all_to_all(
        lax.all_gather(activations, "ba", axis=1, tiled=True),
        "aa", split_axis=1, concat_axis=0, tiled=True,
    )
    return inner_rows(features, lax.all_gather(out_grad, "aa", axis=0, tiled=True))


def plain_direction(scaled):
    row_panel = lax.all_gather(scaled, "ba", axis=1, tiled=True)
    gram_part = inner_rows(row_panel, scaled)
    width = gram_part.shape[0]
    groups = lax.axis_size("aa")
    padding = (groups - width % groups) % groups
    padded = jnp.pad(gram_part, ((0, padding), (0, 0)))
    share = lax.psum_scatter(padded, "aa", scatter_dimension=0, tiled=True).astype(jnp.bfloat16)
    gram_cols = lax.all_gather(share, "aa", axis=0, tiled=True)[:width]
    first_power = jnp.dot(row_panel, gram_cols, preferred_element_type=jnp.float32).astype(
        jnp.bfloat16
    )
    second_power = jnp.dot(
        lax.all_gather(first_power, "ba", axis=1, tiled=True),
        gram_cols,
        preferred_element_type=jnp.float32,
    )
    return (
        3.4445 * scaled.astype(jnp.float32)
        - 4.775 * first_power.astype(jnp.float32)
        + 2.0315 * second_power
    )


def per_device(activations, out_grad, momentum, weight, norm_scale, step_size):
    n, groups = lax.axis_size("ba"), lax.axis_size("aa")
    rows, width = momentum.shape
    tokens, features = activations.shape
    fits = (
        groups == 4 and n == 2 * groups and rows == 2 * features
        and features % 16 == 0 and tokens % 128 == 0 and width % 256 == 0
        and width % (32 * groups) == 0
        and 4 * n * rows * width + 9 * n * width * width + 17 * rows * width < 56 * 2**20
    )
    if fits:
        return fused_step(
            activations, out_grad, momentum, weight, norm_scale, step_size, n, groups
        )
    new_momentum = 0.95 * momentum + plain_gradient(activations, out_grad)
    scaled = (new_momentum / norm_scale).astype(jnp.bfloat16)
    factor = 0.2 * math.sqrt(max(ROWS, COLS))
    new_weight = weight - step_size * factor * plain_direction(scaled)
    return (new_weight, new_momentum)


def solution(mesh):
    placed = (P("aa", "ba"), P("aa", "ba"), P("aa", "ba"), P("aa", "ba"), P(), P())
    return jax.shard_map(
        per_device,
        mesh=mesh,
        in_specs=placed,
        out_specs=(P("aa", "ba"), P("aa", "ba")),
        check_vma=False,
    )
```
